256 devices in a mesh: groups: 4 (over x, y), space: 64 (over z, core).
Axes of the slice: x: 2, y: 2, z: 32, core: 2. Of those that a mesh axis runs over, the one named last changes fastest.
The devices are a block of a 4x8x32 slice.
Arguments:
- hidden: bfloat16 [32768, 512], P(('groups', 'space')), parts along dimension 0, may hold values from -130 to 130
- norm_gain: float32 [512], replicated, may hold values from 0.5 to 2
- norm_shift: float32 [512], replicated, may hold values from -3 to 3
- conv_weight: bfloat16 [3, 3, 3, 512, 512], P(None, None, None, 'space'), may hold values from -0.0546875 to 0.0546875
- conv_bias: bfloat16 [512], replicated, may hold values from -3 to 3
Outputs:
- decoded: bfloat16 [16, 32, 256, 512], P('groups', None, 'space'), parts along dimension 0
The draws below stay inside these ranges and needn't reach their ends.
There are 4 independent parts, one for each index of `groups`. The reference program is written for one: setup_inputs(seed, part) draws one part's arguments, and reference() takes and returns one part's arrays. A program takes and returns all parts, laid end to end along the dimension named above; an argument that names none is the same for every part. Nothing has to cross between parts.
All inputs are finite; a program needn't handle non-finite values.
Results may differ from the reference program's by a relative error of at most 0.0045.
Values may be sent and summed in bfloat16 or wider, within the bound.
No kernel may reach another device: no remote copies, remote signals or barrier semaphores. Data moves between devices by JAX's collectives and lax.ppermute only.
A program may use at most 64 MiB of HBM per device.

```python
import math
import jax
import jax.numpy as jnp
from jax import lax

CHANNELS = 512
GROUPS = 32
FRAMES = 4
ROWS = 16
WIDTH = 128
TOKENS = 8192


def draw_hidden(key, part):
    keys = jax.random.split(jax.random.fold_in(key, 11), 3)
    column = (jnp.arange(TOKENS) % WIDTH).astype(jnp.float32)
    ramp = 1.0 + 2.0 * column / max(WIDTH - 1, 1)
    channel_scale = jnp.exp(jax.random.uniform(keys[1], (CHANNELS,), jnp.float32, 0.0, math.log(10.0)))
    channel_mean = jnp.clip(0.5 * jax.random.normal(keys[2], (CHANNELS,), jnp.float32), -1.5, 1.5)
    base = jnp.clip(jax.random.normal(keys[0], (TOKENS, CHANNELS), jnp.float32), -4.0, 4.0)
    return (base * ramp[:, None] * channel_scale[None, :] + channel_mean[None, :]).astype(jnp.bfloat16)


def level_of(own_key, dims, shards, smallest, high):
    factor_of, own = 1.0, jax.random.fold_in(own_key, 6)
    for axis_at, blocks in shards:
        steps = jnp.exp(jax.random.uniform(jax.random.fold_in(own, axis_at), (blocks,), jnp.float32, smallest / len(shards), high / len(shards)))
        factor_of = factor_of * jnp.repeat(steps, dims[axis_at] // blocks).reshape([-1 if axis == axis_at else 1 for axis in range(len(dims))])
    return factor_of


def bell_draw(own_key, shape, scale, bound, shards=(), dtype=jnp.bfloat16):
    values = scale * jax.random.normal(own_key, shape, jnp.float32)
    if shards:
        values = values * level_of(own_key, shape, shards, -0.22, 0.18)
    return jnp.clip(values, -bound, bound).astype(dtype)


def setup_inputs(seed: int = 0, part: int = 0) -> dict:
    streams_of = jax.random.split(jax.random.key(seed), 6)
    part_keys = jax.random.split(jax.random.fold_in(streams_of[5], part), 6)
    return {
        "hidden": draw_hidden(jax.random.fold_in(jax.random.fold_in(streams_of[5], part), 71), part),
        "norm_gain": jnp.clip(jnp.exp(jax.random.uniform(streams_of[1], (CHANNELS,), jnp.float32, math.log(0.5), math.log(2.0))), 0.5, 2.0),
        "norm_shift": bell_draw(streams_of[2], (CHANNELS,), 0.5, 3.0, (), jnp.float32),
        "conv_weight": bell_draw(streams_of[3], (3, 3, 3, CHANNELS, CHANNELS), (27 * CHANNELS) ** -0.5, 0.0546875, ((3, 64),)),
        "conv_bias": bell_draw(streams_of[4], (CHANNELS,), 0.5, 3.0),
    }


EPSILON = 1e-06

def reference(hidden, norm_gain, norm_shift, conv_weight, conv_bias):
    values = hidden.astype(jnp.float32).reshape(FRAMES, ROWS, WIDTH, GROUPS, CHANNELS // GROUPS)
    average = lax.optimization_barrier(jnp.mean(values, axis=(0, 1, 2, 4), keepdims=True))
    spread = lax.optimization_barrier(jnp.mean((values - average) ** 2, axis=(0, 1, 2, 4), keepdims=True))
    normed = ((values - average) * lax.rsqrt(spread + EPSILON)).reshape(FRAMES, ROWS, WIDTH, CHANNELS)
    active = jax.nn.silu(normed * norm_gain + norm_shift).astype(jnp.bfloat16)
    doubled = jnp.repeat(jnp.repeat(active, 2, axis=1), 2, axis=2)
    padded = jnp.pad(doubled, ((2, 0), (1, 1), (1, 1), (0, 0)), mode='edge')
    result = lax.conv_general_dilated(padded[None].astype(jnp.float32), conv_weight.astype(jnp.float32), (1, 1, 1), 'VALID', dimension_numbers=('NDHWC', 'DHWIO', 'NDHWC'))[0]
    return (result + conv_bias.astype(jnp.float32)).astype(jnp.bfloat16)
```

```python
import functools

import jax
import jax.numpy as jnp
from jax import lax
from jax.experimental import pallas as pl
from jax.experimental.pallas import tpu as pltpu
from jax.sharding import Mesh
from jax.sharding import PartitionSpec as P

CHANNELS = 512
GROUPS = 32
FRAMES = 4
ROWS = 16
COLS = 2
CELLS = FRAMES * ROWS
MEMBERS = CHANNELS // GROUPS
QUAD = 4
SLICE = CHANNELS // QUAD
TAPS = 27
SPACE = ("zh", "zl", "c")
CHIPS = ("zh", "zl")
EPSILON = 1e-06
F32, BF16 = jnp.float32, jnp.bfloat16
HIGHEST = lax.Precision.HIGHEST


def iota(shape, dim):
    return lax.broadcasted_iota(jnp.int32, shape, dim)


def dot(a, b, precision=None):
    return jnp.dot(a, b, preferred_element_type=F32, precision=precision)


def in_pieces(v):
    high = v.astype(BF16)
    rest = v - high.astype(F32)
    middle = rest.astype(BF16)
    low = (rest - middle.astype(F32)).astype(BF16)
    lane = iota(v.shape, 1)
    return jnp.where(
        lane < GROUPS,
        high.astype(F32),
        jnp.where(lane < 2 * GROUPS, middle.astype(F32), low.astype(F32)),
    ).astype(BF16)


def pack_kernel(x_ref, w_ref, o_ref, s_ref):
    quarter = lax.axis_index("gq")
    lanes = pl.ds(pl.multiple_of(quarter * SLICE, SLICE), SLICE)
    s_ref[...] = w_ref[:, :, lanes]
    x = x_ref[...].astype(F32)
    cells = x.shape[0]
    gather = jnp.where(
        (iota((CHANNELS, 128), 0) // MEMBERS == iota((CHANNELS, 128), 1) % GROUPS)
        & (iota((CHANNELS, 128), 1) < 3 * GROUPS),
        1.0,
        0.0,
    )
    spread = jnp.where(iota((128, CHANNELS), 0) == iota((128, CHANNELS), 1) // MEMBERS, 1.0, 0.0)
    sums = jnp.broadcast_to(jnp.sum(x, axis=0, keepdims=True), (8, CHANNELS))
    mean = dot(sums, gather, HIGHEST) * (1.0 / (cells * MEMBERS))
    away = x - dot(mean, spread, HIGHEST)[:1]
    squares = jnp.broadcast_to(jnp.sum(away * away, axis=0, keepdims=True), (8, CHANNELS))
    second = dot(squares, gather, HIGHEST)
    stats = jnp.concatenate([in_pieces(mean)[:1], in_pieces(second)[:1]], axis=0)
    for d in range(cells // COLS):
        o_ref[d, :, :CHANNELS] = x_ref[d * COLS : (d + 1) * COLS, :]
        o_ref[d, :, CHANNELS:] = stats


def norm_kernel(r_ref, gain_ref, shift_ref, o_ref):
    r = r_ref[...].astype(F32)
    rows = r.shape[0]

    def whole(v):
        return v + pltpu.roll(v, 128 - GROUPS, 1) + pltpu.roll(v, 128 - 2 * GROUPS, 1)

    means = whole(r[:, 0, CHANNELS:])
    seconds = whole(r[:, 1, CHANNELS:])
    each = float(rows * COLS * MEMBERS)
    mean = jnp.sum(means, axis=0, keepdims=True) * (1.0 / rows)
    second = jnp.sum(seconds, axis=0, keepdims=True) + each * jnp.sum(
        (means - mean) * (means - mean), axis=0, keepdims=True
    )
    real = iota((1, 128), 1) < GROUPS
    mean = jnp.where(real, mean, 0.0)
    scale = lax.rsqrt(jnp.where(real, second, 0.0) * (1.0 / (each * rows)) + EPSILON)
    spread = jnp.where(iota((128, CHANNELS), 0) == iota((128, CHANNELS), 1) // MEMBERS, 1.0, 0.0)
    mean = dot(jnp.broadcast_to(mean, (8, 128)), spread, HIGHEST)[:1]
    scale = dot(jnp.broadcast_to(scale, (8, 128)), spread, HIGHEST)[:1] * gain_ref[...]
    for j in range(COLS):
        v = (r[:, j, :CHANNELS] - mean) * scale + shift_ref[...]
        o_ref[j] = (v / (1.0 + jnp.exp(-v))).astype(BF16)


def conv_kernel(xa_ref, xl_ref, xr_ref, b_ref, *rest):
    parts, (o_ref, w_ref, x_ref, p0, p1, p2, sem) = rest[:6], rest[6:]
    core, parity, quarter = (lax.axis_index(n) for n in ("c", "zl", "gq"))
    place = lax.axis_index(SPACE)
    last = lax.axis_size(SPACE) - 1
    copies = []
    for n, part in enumerate(parts):
        owner = core if n < 3 else 1 - core
        for j in range(part.shape[0]):
            chip = 2 * (j + (part.shape[0] if n % 3 == 2 else 0)) + (parity if n % 3 == 0 else 1 - parity)
            copies.append(pltpu.make_async_copy(part.at[j], w_ref.at[:, 2 * chip + owner], sem))
    for copy in copies:
        copy.start()

    half = QUAD * CELLS
    for v in range(QUAD):
        blocks = (
            (v * CELLS, jnp.where(place == 0, xa_ref[v, 0], xl_ref[v])),
            (half + v * 2 * CELLS, xa_ref[v, 0]),
            (half + (v * 2 + 1) * CELLS, xa_ref[v, 1]),
            (3 * half + v * CELLS, jnp.where(place == last, xa_ref[v, 1], xr_ref[v])),
        )
        for start, block in blocks:
            for a in range(3):
                for f in range(FRAMES):
                    g = max(f + a - 2, 0)
                    x_ref[a, start + f * ROWS : start + (f + 1) * ROWS] = block[g * ROWS : (g + 1) * ROWS]
    for copy in copies:
        copy.wait()

    taps = w_ref.reshape(TAPS, CHANNELS, SLICE)
    for e, (p_ref, lo, hi) in enumerate(((p0, 0, 3 * half), (p1, half, 3 * half), (p2, half, 4 * half))):
        for rows in ((0, 1), (2,)):
            total = 0.0
            for a in range(3):
                w = jnp.concatenate([taps[a * 9 + b * 3 + e] for b in rows], axis=1)
                total += dot(x_ref[a, lo:hi], w)
            for n, b in enumerate(rows):
                p_ref[b] = total[:, n * SLICE : (n + 1) * SLICE]

    bias = b_ref[pl.ds(quarter, 1)]
    row = iota((CELLS, SLICE), 0) % ROWS

    def combine(v, _):
        def own(p_ref, lead, b, j):
            return p_ref[b, pl.ds(pl.multiple_of(lead + v * 2 * CELLS + j * CELLS, CELLS), CELLS)]

        def edge(p_ref, lead, b):
            return p_ref[b, pl.ds(pl.multiple_of(lead + v * CELLS, CELLS), CELLS)]

        for j in range(COLS):
            for side in range(2):
                t = []
                for b in range(3):
                    if side == 0:
                        first = edge(p0, 0, b) if j == 0 else own(p0, half, b, 0)
                        t.append(first + own(p1, 0, b, j) + own(p2, 0, b, j))
                    else:
                        final = edge(p2, 2 * half, b) if j == 1 else own(p2, 0, b, 1)
                        t.append(own(p0, half, b, j) + own(p1, 0, b, j) + final)
                above = jnp.where(row == 0, t[0], pltpu.roll(t[0], 1, 0))
                below = jnp.where(row == ROWS - 1, t[2], pltpu.roll(t[2], CELLS - 1, 0))
                for up, value in enumerate((above + t[1] + t[2], t[0] + t[1] + below)):
                    at = (up * 2 * COLS + 2 * j + side) * CELLS
                    o_ref[v, at : at + CELLS] = (value + bias).astype(BF16)
        return 0

    lax.fori_loop(0, QUAD, combine, 0)


def vmem(n):
    return [pl.BlockSpec(memory_space=pltpu.VMEM)] * n


def shards(hidden, norm_gain, norm_shift, conv_weight, conv_bias):
    devices = lax.axis_size(SPACE)
    chips = lax.axis_size(CHIPS)
    share = conv_weight.shape[3]
    packed, mine = pl.pallas_call(
        pack_kernel,
        out_shape=(
            jax.ShapeDtypeStruct((devices, COLS, CHANNELS + 128), BF16),
            jax.ShapeDtypeStruct((TAPS, share, SLICE), BF16),
        ),
        in_specs=vmem(2),
        out_specs=tuple(vmem(2)),
        name="pack",
    )(hidden, conv_weight.reshape(TAPS, share, CHANNELS))

    tiles = lax.all_to_all(packed, SPACE, split_axis=0, concat_axis=0, tiled=True)
    kin = lax.all_gather(mine, "zh", axis=0)

    swap = [(0, 1), (1, 0)]
    up = [(i, (i + 1) % chips) for i in range(chips)]
    down = [(j, i) for i, j in up]
    part = kin.shape[0] // 2
    low = lax.ppermute(kin[:part], CHIPS, up)
    high = lax.ppermute(kin[part:], CHIPS, down)
    weights = (kin, low, high)
    weights += tuple(lax.ppermute(w, "c", swap) for w in weights)

    active = pl.pallas_call(
        norm_kernel,
        out_shape=jax.ShapeDtypeStruct((COLS, CELLS, CHANNELS), BF16),
        in_specs=vmem(3),
        out_specs=vmem(1)[0],
        name="norm",
    )(tiles, norm_gain[None], norm_shift[None])
    active = lax.all_gather(active, "gq", axis=0)
    right = [(i, i + 1) for i in range(devices - 1)]
    left = [(j, i) for i, j in right]
    before = lax.ppermute(active[:, 1], SPACE, right)
    after = lax.ppermute(active[:, 0], SPACE, left)

    half = QUAD * CELLS
    out = pl.pallas_call(
        conv_kernel,
        out_shape=jax.ShapeDtypeStruct((QUAD, 4 * COLS * CELLS, SLICE), BF16),
        in_specs=vmem(4) + [pl.BlockSpec(memory_space=pltpu.HBM)] * 6,
        out_specs=vmem(1)[0],
        scratch_shapes=[
            pltpu.VMEM((TAPS, CHANNELS // share, share, SLICE), BF16),
            pltpu.VMEM((3, 4 * half, CHANNELS), BF16),
            pltpu.VMEM((3, 3 * half, SLICE), F32),
            pltpu.VMEM((3, 2 * half, SLICE), F32),
            pltpu.VMEM((3, 3 * half, SLICE), F32),
            pltpu.SemaphoreType.DMA,
        ],
        name="conv",
    )(active, before, after, conv_bias.astype(F32).reshape(QUAD, SLICE), *weights)
    out = lax.all_to_all(out, "gq", split_axis=0, concat_axis=0, tiled=True)
    out = out.reshape(QUAD, 2, 2 * COLS, FRAMES, ROWS, SLICE)
    out = out.transpose(3, 4, 1, 2, 0, 5)
    return out.reshape(FRAMES, 2 * ROWS, 2 * COLS, CHANNELS)


def solution(mesh):
    groups, space = mesh.shape["groups"], mesh.shape["space"]
    torus = Mesh(
        mesh.devices.reshape(groups // QUAD, QUAD, space // 4, 2, 2), ("gh", "gq", "zh", "zl", "c")
    )
    return jax.shard_map(
        shards,
        mesh=torus,
        in_specs=(
            P(("gh", "gq") + SPACE, None),
            P(),
            P(),
            P(None, None, None, SPACE, None),
            P(),
        ),
        out_specs=P(("gh", "gq"), None, SPACE, None),
        check_vma=False,
    )
```

```python
import functools

import jax
import jax.numpy as jnp
from jax import lax
from jax.experimental import pallas as pl
from jax.experimental.pallas import tpu as pltpu
from jax.sharding import Mesh
from jax.sharding import PartitionSpec as P

CHANNELS = 512
GROUPS = 32
FRAMES = 4
ROWS = 16
COLS = 2
CELLS = FRAMES * ROWS
MEMBERS = CHANNELS // GROUPS
QUAD = 4
SLICE = CHANNELS // QUAD
TAPS = 27
SPACE = ("zh", "zl", "c")
CHIPS = ("zh", "zl")
EPSILON = 1e-06
F32, BF16 = jnp.float32, jnp.bfloat16
HIGHEST = lax.Precision.HIGHEST


def iota(shape, dim):
    return lax.broadcasted_iota(jnp.int32, shape, dim)


def dot(a, b, precision=None):
    return jnp.dot(a, b, preferred_element_type=F32, precision=precision)


def in_pieces(v):
    high = v.astype(BF16)
    rest = v - high.astype(F32)
    middle = rest.astype(BF16)
    low = (rest - middle.astype(F32)).astype(BF16)
    lane = iota(v.shape, 1)
    return jnp.where(
        lane < GROUPS,
        high.astype(F32),
        jnp.where(lane < 2 * GROUPS, middle.astype(F32), low.astype(F32)),
    ).astype(BF16)


def pack_kernel(x_ref, w_ref, o_ref, s_ref):
    quarter = lax.axis_index("gq")
    lanes = pl.ds(pl.multiple_of(quarter * SLICE, SLICE), SLICE)
    s_ref[...] = w_ref[:, :, lanes]
    x = x_ref[...].astype(F32)
    cells = x.shape[0]
    gather = jnp.where(
        (iota((CHANNELS, 128), 0) // MEMBERS == iota((CHANNELS, 128), 1) % GROUPS)
        & (iota((CHANNELS, 128), 1) < 3 * GROUPS),
        1.0,
        0.0,
    )
    spread = jnp.where(iota((128, CHANNELS), 0) == iota((128, CHANNELS), 1) // MEMBERS, 1.0, 0.0)
    sums = jnp.broadcast_to(jnp.sum(x, axis=0, keepdims=True), (8, CHANNELS))
    mean = dot(sums, gather, HIGHEST) * (1.0 / (cells * MEMBERS))
    away = x - dot(mean, spread, HIGHEST)[:1]
    squares = jnp.broadcast_to(jnp.sum(away * away, axis=0, keepdims=True), (8, CHANNELS))
    second = dot(squares, gather, HIGHEST)
    stats = jnp.concatenate([in_pieces(mean)[:1], in_pieces(second)[:1]], axis=0)
    for d in range(cells // COLS):
        o_ref[d, :, :CHANNELS] = x_ref[d * COLS : (d + 1) * COLS, :]
        o_ref[d, :, CHANNELS:] = stats


def norm_kernel(r_ref, gain_ref, shift_ref, o_ref):
    r = r_ref[...].astype(F32)
    rows = r.shape[0]

    def whole(v):
        return v + pltpu.roll(v, 128 - GROUPS, 1) + pltpu.roll(v, 128 - 2 * GROUPS, 1)

    means = whole(r[:, 0, CHANNELS:])
    seconds = whole(r[:, 1, CHANNELS:])
    each = float(rows * COLS * MEMBERS)
    mean = jnp.sum(means, axis=0, keepdims=True) * (1.0 / rows)
    second = jnp.sum(seconds, axis=0, keepdims=True) + each * jnp.sum(
        (means - mean) * (means - mean), axis=0, keepdims=True
    )
    real = iota((1, 128), 1) < GROUPS
    mean = jnp.where(real, mean, 0.0)
    scale = lax.rsqrt(jnp.where(real, second, 0.0) * (1.0 / (each * rows)) + EPSILON)
    spread = jnp.where(iota((128, CHANNELS), 0) == iota((128, CHANNELS), 1) // MEMBERS, 1.0, 0.0)
    mean = dot(jnp.broadcast_to(mean, (8, 128)), spread, HIGHEST)[:1]
    scale = dot(jnp.broadcast_to(scale, (8, 128)), spread, HIGHEST)[:1] * gain_ref[...]
    for j in range(COLS):
        v = (r[:, j, :CHANNELS] - mean) * scale + shift_ref[...]
        o_ref[j] = (v / (1.0 + jnp.exp(-v))).astype(BF16)


def conv_kernel(xa_ref, xl_ref, xr_ref, b_ref, *rest):
    parts, (o_ref, w_ref, x_ref, p0, p1, p2, y_ref, sem) = rest[:6], rest[6:]
    core, parity, quarter = (lax.axis_index(n) for n in ("c", "zl", "gq"))
    place = lax.axis_index(SPACE)
    last = lax.axis_size(SPACE) - 1
    copies = []
    for n, part in enumerate(parts):
        owner = core if n < 3 else 1 - core
        for j in range(part.shape[0]):
            chip = 2 * (j + (part.shape[0] if n % 3 == 2 else 0)) + (parity if n % 3 == 0 else 1 - parity)
            copies.append(pltpu.make_async_copy(part.at[j], w_ref.at[:, 2 * chip + owner], sem))
    for copy in copies:
        copy.start()

    half = QUAD * CELLS
    for v in range(QUAD):
        blocks = (
            (v * CELLS, jnp.where(place == 0, xa_ref[v, 0], xl_ref[v])),
            (half + v * 2 * CELLS, xa_ref[v, 0]),
            (half + (v * 2 + 1) * CELLS, xa_ref[v, 1]),
            (3 * half + v * CELLS, jnp.where(place == last, xa_ref[v, 1], xr_ref[v])),
        )
        for start, block in blocks:
            for a in range(3):
                for f in range(FRAMES):
                    g = max(f + a - 2, 0)
                    x_ref[a, start + f * ROWS : start + (f + 1) * ROWS] = block[g * ROWS : (g + 1) * ROWS]
    for copy in copies:
        copy.wait()

    taps = w_ref.reshape(TAPS, CHANNELS, SLICE)
    for e, (p_ref, lo, hi) in enumerate(((p0, 0, 3 * half), (p1, half, 3 * half), (p2, half, 4 * half))):
        for rows in ((0, 1), (2,)):
            total = 0.0
            for a in range(3):
                w = jnp.concatenate([taps[a * 9 + b * 3 + e] for b in rows], axis=1)
                total += dot(x_ref[a, lo:hi], w)
            for n, b in enumerate(rows):
                p_ref[b] = total[:, n * SLICE : (n + 1) * SLICE]

    bias = b_ref[pl.ds(quarter, 1)]
    row = iota((CELLS, SLICE), 0) % ROWS

    def combine(v, _):
        def own(p_ref, lead, b, j):
            return p_ref[b, pl.ds(pl.multiple_of(lead + v * 2 * CELLS + j * CELLS, CELLS), CELLS)]

        def edge(p_ref, lead, b):
            return p_ref[b, pl.ds(pl.multiple_of(lead + v * CELLS, CELLS), CELLS)]

        for j in range(COLS):
            for side in range(2):
                t = []
                for b in range(3):
                    if side == 0:
                        first = edge(p0, 0, b) if j == 0 else own(p0, half, b, 0)
                        t.append(first + own(p1, 0, b, j) + own(p2, 0, b, j))
                    else:
                        final = edge(p2, 2 * half, b) if j == 1 else own(p2, 0, b, 1)
                        t.append(own(p0, half, b, j) + own(p1, 0, b, j) + final)
                above = jnp.where(row == 0, t[0], pltpu.roll(t[0], 1, 0))
                below = jnp.where(row == ROWS - 1, t[2], pltpu.roll(t[2], CELLS - 1, 0))
                for up, value in enumerate((above + t[1] + t[2], t[0] + t[1] + below)):
                    at = up * 2 * COLS + 2 * j + side
                    y_ref[pl.ds(at, CELLS, stride=4 * COLS), :] = value + bias
        o_ref[v] = y_ref[...].reshape(2 * CELLS, 2 * COLS, SLICE).astype(BF16)
        return 0

    lax.fori_loop(0, QUAD, combine, 0)


def spread_kernel(i_ref, o_ref, sem):
    copies = [
        pltpu.make_async_copy(i_ref.at[q], o_ref.at[:, :, pl.ds(q * SLICE, SLICE)], sem)
        for q in range(QUAD)
    ]
    for copy in copies:
        copy.start()
    for copy in copies:
        copy.wait()


def room(mebibytes):
    return pltpu.CompilerParams(vmem_limit_bytes=mebibytes * 2**20)


def vmem(n):
    return [pl.BlockSpec(memory_space=pltpu.VMEM)] * n


def shards(hidden, norm_gain, norm_shift, conv_weight, conv_bias):
    devices = lax.axis_size(SPACE)
    chips = lax.axis_size(CHIPS)
    share = conv_weight.shape[3]
    packed, mine = pl.pallas_call(
        pack_kernel,
        out_shape=(
            jax.ShapeDtypeStruct((devices, COLS, CHANNELS + 128), BF16),
            jax.ShapeDtypeStruct((TAPS, share, SLICE), BF16),
        ),
        in_specs=vmem(2),
        out_specs=tuple(vmem(2)),
        compiler_params=room(4),
        name="pack",
    )(hidden, conv_weight.reshape(TAPS, share, CHANNELS))

    tiles = lax.all_to_all(packed, SPACE, split_axis=0, concat_axis=0, tiled=True)
    kin = lax.all_gather(mine, "zh", axis=0)

    swap = [(0, 1), (1, 0)]
    up = [(i, (i + 1) % chips) for i in range(chips)]
    down = [(j, i) for i, j in up]
    part = kin.shape[0] // 2
    low = lax.ppermute(kin[:part], CHIPS, up)
    high = lax.ppermute(kin[part:], CHIPS, down)
    active = pl.pallas_call(
        norm_kernel,
        out_shape=jax.ShapeDtypeStruct((COLS, CELLS, CHANNELS), BF16),
        in_specs=vmem(3),
        out_specs=vmem(1)[0],
        compiler_params=room(4),
        name="norm",
    )(tiles, norm_gain[None], norm_shift[None])
    active = lax.all_gather(active, "gq", axis=0)
    active, low, high = lax.optimization_barrier((active, low, high))
    weights = (kin, low, high)
    weights += tuple(lax.ppermute(w, "c", swap) for w in weights)
    right = [(i, i + 1) for i in range(devices - 1)]
    left = [(j, i) for i, j in right]
    before = lax.ppermute(active[:, 1], SPACE, right)
    after = lax.ppermute(active[:, 0], SPACE, left)

    half = QUAD * CELLS
    out = pl.pallas_call(
        conv_kernel,
        out_shape=jax.ShapeDtypeStruct((QUAD, 2 * CELLS, 2 * COLS, SLICE), BF16),
        in_specs=vmem(4) + [pl.BlockSpec(memory_space=pltpu.HBM)] * 6,
        out_specs=vmem(1)[0],
        scratch_shapes=[
            pltpu.VMEM((TAPS, CHANNELS // share, share, SLICE), BF16),
            pltpu.VMEM((3, 4 * half, CHANNELS), BF16),
            pltpu.VMEM((3, 3 * half, SLICE), F32),
            pltpu.VMEM((3, 2 * half, SLICE), F32),
            pltpu.VMEM((3, 3 * half, SLICE), F32),
            pltpu.VMEM((4 * COLS * CELLS, SLICE), F32),
            pltpu.SemaphoreType.DMA,
        ],
        compiler_params=room(24),
        name="conv",
    )(active, before, after, conv_bias.astype(F32).reshape(QUAD, SLICE), *weights)
    out = lax.all_to_all(out, "gq", split_axis=0, concat_axis=0, tiled=True)
    out = pl.pallas_call(
        spread_kernel,
        out_shape=jax.ShapeDtypeStruct((2 * CELLS, 2 * COLS, CHANNELS), BF16),
        in_specs=vmem(1),
        out_specs=pl.BlockSpec(memory_space=pltpu.HBM),
        scratch_shapes=[pltpu.SemaphoreType.DMA],
        compiler_params=room(4),
        name="spread",
    )(out)
    return out.reshape(FRAMES, 2 * ROWS, 2 * COLS, CHANNELS)


def solution(mesh):
    groups, space = mesh.shape["groups"], mesh.shape["space"]
    torus = Mesh(
        mesh.devices.reshape(groups // QUAD, QUAD, space // 4, 2, 2), ("gh", "gq", "zh", "zl", "c")
    )
    return jax.shard_map(
        shards,
        mesh=torus,
        in_specs=(
            P(("gh", "gq") + SPACE, None),
            P(),
            P(),
            P(None, None, None, SPACE, None),
            P(),
        ),
        out_specs=P(("gh", "gq"), None, SPACE, None),
        check_vma=False,
    )
```

```python
import jax
import jax.numpy as jnp
from jax import lax
from jax.experimental import pallas as pl
from jax.experimental.pallas import tpu as pltpu
from jax.sharding import Mesh
from jax.sharding import PartitionSpec as P

CHANNELS = 512
GROUPS = 32
FRAMES = 4
ROWS = 16
COLS = 2
WIDE = 2 * COLS
CLASSES = 4
CELLS = FRAMES * ROWS
MEMBERS = CHANNELS // GROUPS
QUAD = 4
SLICE = CHANNELS // QUAD
TAPS = 27
SPACE = ("zh", "zl", "c")
CHIPS = ("zh", "zl")
EPSILON = 1e-06
F32, BF16 = jnp.float32, jnp.bfloat16
HIGHEST = lax.Precision.HIGHEST


def iota(shape, dim):
    return lax.broadcasted_iota(jnp.int32, shape, dim)


def dot(a, b, precision=None):
    return jnp.dot(a, b, preferred_element_type=F32, precision=precision)


def in_pieces(v):
    high = v.astype(BF16)
    rest = v - high.astype(F32)
    middle = rest.astype(BF16)
    low = (rest - middle.astype(F32)).astype(BF16)
    lane = iota(v.shape, 1)
    return jnp.where(
        lane < GROUPS,
        high.astype(F32),
        jnp.where(lane < 2 * GROUPS, middle.astype(F32), low.astype(F32)),
    ).astype(BF16)


def pack_kernel(x_ref, y_ref, o_ref):
    rows = [ref[...].astype(F32) for ref in (x_ref, y_ref)]
    cells = x_ref.shape[0]
    gather = jnp.where(
        (iota((CHANNELS, 128), 0) // MEMBERS == iota((CHANNELS, 128), 1) % GROUPS)
        & (iota((CHANNELS, 128), 1) < 3 * GROUPS),
        1.0,
        0.0,
    )
    spread = jnp.where(iota((128, CHANNELS), 0) == iota((128, CHANNELS), 1) // MEMBERS, 1.0, 0.0)

    def totals(values):
        return jnp.broadcast_to(sum(jnp.sum(v, axis=0, keepdims=True) for v in values), (8, CHANNELS))

    mean = dot(totals(rows), gather, HIGHEST) * (1.0 / (2 * cells * MEMBERS))
    away = [v - dot(mean, spread, HIGHEST)[:1] for v in rows]
    second = dot(totals([v * v for v in away]), gather, HIGHEST)
    stats = jnp.concatenate([in_pieces(mean)[:1], in_pieces(second)[:1]], axis=0)
    for d in range(cells // WIDE):
        for j in range(WIDE):
            c = d * WIDE + j
            pair = jnp.concatenate([v[c : c + 1] for v in rows], axis=0)
            o_ref[d, :, j * CHANNELS : (j + 1) * CHANNELS] = pair.astype(BF16)
        o_ref[d, :, WIDE * CHANNELS :] = stats


def norm_kernel(r_ref, gain_ref, shift_ref, o_ref):
    r = r_ref[...].astype(F32)
    sources = r.shape[0]

    def whole(v):
        return v + pltpu.roll(v, 128 - GROUPS, 1) + pltpu.roll(v, 128 - 2 * GROUPS, 1)

    means = whole(r[:, 0, WIDE * CHANNELS :])
    seconds = whole(r[:, 1, WIDE * CHANNELS :])
    each = float(2 * sources * WIDE * MEMBERS)
    mean = jnp.sum(means, axis=0, keepdims=True) * (1.0 / sources)
    second = jnp.sum(seconds, axis=0, keepdims=True) + each * jnp.sum(
        (means - mean) * (means - mean), axis=0, keepdims=True
    )
    real = iota((1, 128), 1) < GROUPS
    mean = jnp.where(real, mean, 0.0)
    scale = lax.rsqrt(jnp.where(real, second, 0.0) * (1.0 / (each * sources)) + EPSILON)
    spread = jnp.where(iota((128, CHANNELS), 0) == iota((128, CHANNELS), 1) // MEMBERS, 1.0, 0.0)
    mean = dot(jnp.broadcast_to(mean, (8, 128)), spread, HIGHEST)[:1]
    scale = dot(jnp.broadcast_to(scale, (8, 128)), spread, HIGHEST)[:1] * gain_ref[...]
    for j in range(WIDE):
        x = r[:, :, j * CHANNELS : (j + 1) * CHANNELS].reshape(2 * sources, CHANNELS)
        v = (x - mean) * scale + shift_ref[...]
        o_ref[j] = (v / (1.0 + jnp.exp(-v))).astype(BF16)


def slice_kernel(x_ref, y_ref, o_ref):
    quarter = lax.axis_index("gq")
    lanes = pl.ds(pl.multiple_of(quarter * SLICE, SLICE), SLICE)
    share = x_ref.shape[1]
    o_ref[:, :share] = x_ref[:, :, lanes]
    o_ref[:, share:] = y_ref[:, :, lanes]


def conv_kernel(xa_ref, xl_ref, xr_ref, ya_ref, yr_ref, b_ref, *rest):
    parts = (rest[:2], rest[2:4])
    o_ref, w_ref, x_ref, p0, p1, p2, y_ref, sem = rest[4:]
    core, kind, quarter = (lax.axis_index(n) for n in ("c", "zl", "gq"))
    rows = w_ref.shape[1] // CLASSES
    away = (0, CLASSES - 1, 1, 2)

    def copies(pieces):
        made = []
        for n in range(CLASSES):
            for j in range(rows):
                part = pieces[0].at[n * rows + j] if n < CLASSES - 1 else pieces[1].at[j]
                chip = CLASSES * j + lax.rem(kind + away[n], CLASSES)
                made.append(pltpu.make_async_copy(part, w_ref.at[:, chip], sem))
        return made

    for owner in range(2):

        @pl.when(core == owner)
        def _():
            for copy in copies(parts[owner]):
                copy.start()

    half = QUAD * CELLS
    west = core == 0
    place = lax.axis_index(CHIPS)
    final = lax.axis_size(CHIPS) - 1
    for v in range(QUAD):
        inner = [jnp.where(west, xa_ref[j, v], ya_ref[COLS + j, v]) for j in range(COLS)]
        outer = jnp.where(west, jnp.where(place == 0, xa_ref[0, v], xl_ref[v]), ya_ref[1, v])
        other = jnp.where(
            west, xa_ref[COLS, v], jnp.where(place == final, ya_ref[WIDE - 1, v], yr_ref[v])
        )
        blocks = (
            (v * CELLS, outer),
            (half + v * 2 * CELLS, inner[0]),
            (half + (v * 2 + 1) * CELLS, inner[1]),
            (3 * half + v * CELLS, other),
        )
        for start, block in blocks:
            for a in range(3):
                for f in range(FRAMES):
                    g = max(f + a - 2, 0)
                    x_ref[a, start + f * ROWS : start + (f + 1) * ROWS] = block[g * ROWS : (g + 1) * ROWS]
    for copy in copies(parts[0]):
        copy.wait()

    taps = w_ref.reshape(TAPS, CHANNELS, SLICE)
    for e, (p_ref, lo, hi) in enumerate(((p0, 0, 3 * half), (p1, half, 3 * half), (p2, half, 4 * half))):
        for rows in ((0, 1), (2,)):
            total = 0.0
            for a in range(3):
                w = jnp.concatenate([taps[a * 9 + b * 3 + e] for b in rows], axis=1)
                total += dot(x_ref[a, lo:hi], w)
            for n, b in enumerate(rows):
                p_ref[b] = total[:, n * SLICE : (n + 1) * SLICE]

    bias = b_ref[pl.ds(quarter, 1)]
    row = iota((CELLS, SLICE), 0) % ROWS

    def combine(v, _):
        def own(p_ref, lead, b, j):
            return p_ref[b, pl.ds(pl.multiple_of(lead + v * 2 * CELLS + j * CELLS, CELLS), CELLS)]

        def edge(p_ref, lead, b):
            return p_ref[b, pl.ds(pl.multiple_of(lead + v * CELLS, CELLS), CELLS)]

        for j in range(COLS):
            for side in range(2):
                t = []
                for b in range(3):
                    if side == 0:
                        first = edge(p0, 0, b) if j == 0 else own(p0, half, b, 0)
                        t.append(first + own(p1, 0, b, j) + own(p2, 0, b, j))
                    else:
                        final = edge(p2, 2 * half, b) if j == 1 else own(p2, 0, b, 1)
                        t.append(own(p0, half, b, j) + own(p1, 0, b, j) + final)
                above = jnp.where(row == 0, t[0], pltpu.roll(t[0], 1, 0))
                below = jnp.where(row == ROWS - 1, t[2], pltpu.roll(t[2], CELLS - 1, 0))
                for up, value in enumerate((above + t[1] + t[2], t[0] + t[1] + below)):
                    at = up * 2 * COLS + 2 * j + side
                    y_ref[pl.ds(at, CELLS, stride=4 * COLS), :] = value + bias
        o_ref[quarter ^ v] = y_ref[...].reshape(2 * CELLS, 2 * COLS, SLICE).astype(BF16)
        return 0

    lax.fori_loop(0, QUAD, combine, 0)


def spread_kernel(i_ref, o_ref, sem):
    copies = [
        pltpu.make_async_copy(i_ref.at[q], o_ref.at[:, :, pl.ds(q * SLICE, SLICE)], sem)
        for q in range(QUAD)
    ]
    for copy in copies:
        copy.start()
    for copy in copies:
        copy.wait()


def room(mebibytes):
    return pltpu.CompilerParams(vmem_limit_bytes=mebibytes * 2**20)


def vmem(n):
    return [pl.BlockSpec(memory_space=pltpu.VMEM)] * n


def shards(hidden, norm_gain, norm_shift, conv_weight, conv_bias):
    chips = lax.axis_size(CHIPS)
    share = 2 * conv_weight.shape[3]
    weight = conv_weight.reshape(TAPS, share // 2, CHANNELS)
    rows = lax.axis_size("zh")
    width = WIDE * CHANNELS + 128
    token = lax.ppermute(hidden, "c", [(1, 0)])
    other = lax.ppermute(weight, "c", [(0, 1)])

    column = (QUAD, CELLS, CHANNELS)
    act_shape = (WIDE,) + column
    kin_shapes = tuple((n * rows, TAPS, share, SLICE) for n in (CLASSES - 1, 1))

    def blank(*shapes):
        return pl.pallas_call(
            lambda *refs: None,
            out_shape=tuple(jax.ShapeDtypeStruct(shape, BF16) for shape in shapes),
            out_specs=tuple(pl.BlockSpec(memory_space=pl.ANY) for _ in shapes),
            compiler_params=room(1),
            name="blank",
        )()

    def ring(step):
        return [(i, (i + step) % chips) for i in range(chips)]

    def activations(hidden, token, weight, other):
        packed = pl.pallas_call(
            pack_kernel,
            out_shape=jax.ShapeDtypeStruct((chips, 2, width), BF16),
            in_specs=vmem(2),
            out_specs=vmem(1)[0],
            compiler_params=room(6),
            name="pack",
        )(hidden, token)
        tiles = lax.all_to_all(packed, CHIPS, split_axis=0, concat_axis=0, tiled=True)
        active = pl.pallas_call(
            norm_kernel,
            out_shape=jax.ShapeDtypeStruct((WIDE, CELLS, CHANNELS), BF16),
            in_specs=vmem(3),
            out_specs=vmem(1)[0],
            compiler_params=room(6),
            name="norm",
        )(tiles, norm_gain[None], norm_shift[None])
        videos = [active]
        for n in range(1, QUAD):
            videos.append(lax.ppermute(active, "gq", [(i, i ^ n) for i in range(QUAD)]))
        return (jnp.stack(videos, axis=1),) + blank(*kin_shapes)

    def kernels(hidden, token, weight, other):
        mine = pl.pallas_call(
            slice_kernel,
            out_shape=jax.ShapeDtypeStruct((TAPS, share, SLICE), BF16),
            in_specs=vmem(2),
            out_specs=vmem(1)[0],
            compiler_params=room(4),
            name="slice",
        )(other, weight)
        kin = lax.all_gather(mine, "zh", axis=0)
        below = lax.ppermute(kin, CHIPS, ring(1))
        above = lax.ppermute(kin, CHIPS, ring(-1))
        low = lax.ppermute(below[: rows // 2], CHIPS, ring(1))
        high = lax.ppermute(above[rows // 2 :], CHIPS, ring(-1))
        near = jnp.concatenate([kin, below, above], axis=0)
        return blank(act_shape) + (near, jnp.concatenate([low, high], axis=0))

    core = lax.axis_index("c")
    active, near, far = lax.cond(core == 0, activations, kernels, hidden, token, weight, other)
    right = [(2 * i, 2 * i + 2) for i in range(chips - 1)]
    left = [(j, i) for i, j in right]
    before = lax.ppermute(active[WIDE - 1], SPACE, right)
    after = lax.ppermute(active[0], SPACE, left)
    given = lax.ppermute(active, "c", [(0, 1)])
    weights = (near, far)
    weights = tuple(lax.ppermute(w, "c", [(1, 0)]) for w in weights) + weights
    acts = (active, before, after, given, lax.ppermute(after, "c", [(0, 1)]))

    half = QUAD * CELLS
    out = pl.pallas_call(
        conv_kernel,
        out_shape=jax.ShapeDtypeStruct((QUAD, 2 * CELLS, 2 * COLS, SLICE), BF16),
        in_specs=vmem(6) + [pl.BlockSpec(memory_space=pltpu.HBM)] * 4,
        out_specs=vmem(1)[0],
        scratch_shapes=[
            pltpu.VMEM((TAPS, chips, share, SLICE), BF16),
            pltpu.VMEM((3, 4 * half, CHANNELS), BF16),
            pltpu.VMEM((3, 3 * half, SLICE), F32),
            pltpu.VMEM((3, 2 * half, SLICE), F32),
            pltpu.VMEM((3, 3 * half, SLICE), F32),
            pltpu.VMEM((4 * COLS * CELLS, SLICE), F32),
            pltpu.SemaphoreType.DMA,
        ],
        compiler_params=room(24),
        name="conv",
    )(*acts, conv_bias.astype(F32).reshape(QUAD, SLICE), *weights)
    out = lax.all_to_all(out, "gq", split_axis=0, concat_axis=0, tiled=True)
    out = pl.pallas_call(
        spread_kernel,
        out_shape=jax.ShapeDtypeStruct((2 * CELLS, 2 * COLS, CHANNELS), BF16),
        in_specs=vmem(1),
        out_specs=pl.BlockSpec(memory_space=pltpu.HBM),
        scratch_shapes=[pltpu.SemaphoreType.DMA],
        compiler_params=room(4),
        name="spread",
    )(out)
    return out.reshape(FRAMES, 2 * ROWS, 2 * COLS, CHANNELS)


def solution(mesh):
    groups, space = mesh.shape["groups"], mesh.shape["space"]
    torus = Mesh(
        mesh.devices.reshape(groups // QUAD, QUAD, space // (2 * CLASSES), CLASSES, 2),
        ("gh", "gq", "zh", "zl", "c"),
    )
    return jax.shard_map(
        shards,
        mesh=torus,
        in_specs=(
            P(("gh", "gq") + SPACE, None),
            P(),
            P(),
            P(None, None, None, SPACE, None),
            P(),
        ),
        out_specs=P(("gh", "gq"), None, SPACE, None),
        check_vma=False,
    )
```

```python
import jax
import jax.numpy as jnp
from jax import lax
from jax.experimental import pallas as pl
from jax.experimental.pallas import tpu as pltpu
from jax.sharding import Mesh
from jax.sharding import PartitionSpec as P

CHANNELS = 512
GROUPS = 32
FRAMES = 4
ROWS = 16
COLS = 2
WIDE = 2 * COLS
CLASSES = 4
CELLS = FRAMES * ROWS
MEMBERS = CHANNELS // GROUPS
QUAD = 4
SLICE = CHANNELS // QUAD
TAPS = 27
SPACE = ("zh", "zl", "c")
CHIPS = ("zh", "zl")
EPSILON = 1e-06
F32, BF16 = jnp.float32, jnp.bfloat16
HIGHEST = lax.Precision.HIGHEST


def iota(shape, dim):
    return lax.broadcasted_iota(jnp.int32, shape, dim)


def dot(a, b, precision=None):
    return jnp.dot(a, b, preferred_element_type=F32, precision=precision)


def in_pieces(v):
    high = v.astype(BF16)
    rest = v - high.astype(F32)
    middle = rest.astype(BF16)
    low = (rest - middle.astype(F32)).astype(BF16)
    lane = iota(v.shape, 1)
    return jnp.where(
        lane < GROUPS,
        high.astype(F32),
        jnp.where(lane < 2 * GROUPS, middle.astype(F32), low.astype(F32)),
    ).astype(BF16)


def parcel_kernel(x_ref, w_ref, p_ref, s_ref, r_ref, sem):
    core, quarter = lax.axis_index("c"), lax.axis_index("gq")
    lanes = pl.ds(pl.multiple_of(quarter * SLICE, SLICE), SLICE)
    tiles = x_ref.shape[0]

    def token_copies():
        return [
            pltpu.make_async_copy(
                x_ref.at[:, :, pl.ds(n * SLICE, SLICE)], p_ref.at[pl.ds(n * tiles, tiles)], sem.at[2 + n]
            )
            for n in range(CHANNELS // SLICE)
        ]

    def slice_copy():
        return pltpu.make_async_copy(w_ref.at[:, :, lanes], p_ref.at[pl.ds(0, TAPS)], sem.at[2])

    own = pltpu.make_async_copy(w_ref.at[:, :, lanes], s_ref, sem.at[0])
    row = pltpu.make_async_copy(x_ref, r_ref, sem.at[1])

    @pl.when(core == 0)
    def _():
        slice_copy().start()
        row.start()
        slice_copy().wait()
        row.wait()

    @pl.when(core == 1)
    def _():
        for copy in token_copies():
            copy.start()
        own.start()
        for copy in token_copies():
            copy.wait()
        own.wait()


def pack_kernel(x_ref, y_ref, o_ref):
    cells = x_ref.shape[0] * x_ref.shape[1]
    tiles = x_ref.shape[0]
    own = x_ref[...].astype(F32).reshape(cells, CHANNELS)
    given = [
        y_ref[n * tiles : (n + 1) * tiles].astype(F32).reshape(cells, SLICE)
        for n in range(CHANNELS // SLICE)
    ]
    rows = [own, jnp.concatenate(given, axis=1)]
    gather = jnp.where(
        (iota((CHANNELS, 128), 0) // MEMBERS == iota((CHANNELS, 128), 1) % GROUPS)
        & (iota((CHANNELS, 128), 1) < 3 * GROUPS),
        1.0,
        0.0,
    )
    spread = jnp.where(iota((128, CHANNELS), 0) == iota((128, CHANNELS), 1) // MEMBERS, 1.0, 0.0)

    def totals(values):
        return jnp.broadcast_to(sum(jnp.sum(v, axis=0, keepdims=True) for v in values), (8, CHANNELS))

    mean = dot(totals(rows), gather, HIGHEST) * (1.0 / (2 * cells * MEMBERS))
    away = [v - dot(mean, spread, HIGHEST)[:1] for v in rows]
    second = dot(totals([v * v for v in away]), gather, HIGHEST)
    stats = jnp.concatenate([in_pieces(mean)[:1], in_pieces(second)[:1]], axis=0)
    for d in range(cells // WIDE):
        for j in range(WIDE):
            c = d * WIDE + j
            pair = jnp.concatenate([v[c : c + 1] for v in rows], axis=0)
            o_ref[d, :, j * CHANNELS : (j + 1) * CHANNELS] = pair.astype(BF16)
        o_ref[d, :, WIDE * CHANNELS :] = stats


def norm_kernel(r_ref, gain_ref, shift_ref, o_ref):
    r = r_ref[...].astype(F32)
    sources = r.shape[0]

    def whole(v):
        return v + pltpu.roll(v, 128 - GROUPS, 1) + pltpu.roll(v, 128 - 2 * GROUPS, 1)

    means = whole(r[:, 0, WIDE * CHANNELS :])
    seconds = whole(r[:, 1, WIDE * CHANNELS :])
    each = float(2 * sources * WIDE * MEMBERS)
    mean = jnp.sum(means, axis=0, keepdims=True) * (1.0 / sources)
    second = jnp.sum(seconds, axis=0, keepdims=True) + each * jnp.sum(
        (means - mean) * (means - mean), axis=0, keepdims=True
    )
    real = iota((1, 128), 1) < GROUPS
    mean = jnp.where(real, mean, 0.0)
    scale = lax.rsqrt(jnp.where(real, second, 0.0) * (1.0 / (each * sources)) + EPSILON)
    spread = jnp.where(iota((128, CHANNELS), 0) == iota((128, CHANNELS), 1) // MEMBERS, 1.0, 0.0)
    mean = dot(jnp.broadcast_to(mean, (8, 128)), spread, HIGHEST)[:1]
    scale = dot(jnp.broadcast_to(scale, (8, 128)), spread, HIGHEST)[:1] * gain_ref[...]
    for j in range(WIDE):
        x = r[:, :, j * CHANNELS : (j + 1) * CHANNELS].reshape(2 * sources, CHANNELS)
        v = (x - mean) * scale + shift_ref[...]
        o_ref[j] = (v / (1.0 + jnp.exp(-v))).astype(BF16)


def conv_kernel(x0_ref, l0_ref, x1_ref, r1_ref, b_ref, *rest):
    parts = (rest[:2], rest[2:4])
    o_ref, w_ref, x_ref, p0, p1, p2, y_ref, sem = rest[4:]
    core, kind, quarter = (lax.axis_index(n) for n in ("c", "zl", "gq"))
    rows = w_ref.shape[1] // CLASSES
    away = (0, CLASSES - 1, 1, 2)

    def copies(pieces):
        made = []
        for n in range(CLASSES):
            for j in range(rows):
                part = pieces[0].at[n * rows + j] if n < CLASSES - 1 else pieces[1].at[j]
                chip = CLASSES * j + lax.rem(kind + away[n], CLASSES)
                made.append(pltpu.make_async_copy(part, w_ref.at[:, chip], sem))
        return made

    for owner in range(2):

        @pl.when(core == owner)
        def _():
            for copy in copies(parts[owner]):
                copy.start()

    half = QUAD * CELLS
    place = lax.axis_index(CHIPS)
    final = lax.axis_size(CHIPS) - 1
    for v in range(QUAD):
        sides = (
            [jnp.where(place == 0, x0_ref[v, 0], l0_ref[v])] + [x0_ref[v, j] for j in range(WIDE - 1)],
            [x1_ref[v, j] for j in range(WIDE - 1)] + [jnp.where(place == final, x1_ref[v, WIDE - 2], r1_ref[v])],
        )
        outer, first, second, other = (jnp.where(core == 0, x, y) for x, y in zip(*sides))
        blocks = (
            (v * CELLS, outer),
            (half + v * 2 * CELLS, first),
            (half + (v * 2 + 1) * CELLS, second),
            (3 * half + v * CELLS, other),
        )
        for start, block in blocks:
            for a in range(3):
                for f in range(FRAMES):
                    g = max(f + a - 2, 0)
                    x_ref[a, start + f * ROWS : start + (f + 1) * ROWS] = block[g * ROWS : (g + 1) * ROWS]
    for copy in copies(parts[0]):
        copy.wait()

    taps = w_ref.reshape(TAPS, CHANNELS, SLICE)
    for e, (p_ref, lo, hi) in enumerate(((p0, 0, 3 * half), (p1, half, 3 * half), (p2, half, 4 * half))):
        for rows in ((0, 1), (2,)):
            total = 0.0
            for a in range(3):
                w = jnp.concatenate([taps[a * 9 + b * 3 + e] for b in rows], axis=1)
                total += dot(x_ref[a, lo:hi], w)
            for n, b in enumerate(rows):
                p_ref[b] = total[:, n * SLICE : (n + 1) * SLICE]

    bias = b_ref[pl.ds(quarter, 1)]
    row = iota((CELLS, SLICE), 0) % ROWS

    def combine(v, _):
        def own(p_ref, lead, b, j):
            return p_ref[b, pl.ds(pl.multiple_of(lead + v * 2 * CELLS + j * CELLS, CELLS), CELLS)]

        def edge(p_ref, lead, b):
            return p_ref[b, pl.ds(pl.multiple_of(lead + v * CELLS, CELLS), CELLS)]

        for j in range(COLS):
            for side in range(2):
                t = []
                for b in range(3):
                    if side == 0:
                        first = edge(p0, 0, b) if j == 0 else own(p0, half, b, 0)
                        t.append(first + own(p1, 0, b, j) + own(p2, 0, b, j))
                    else:
                        final = edge(p2, 2 * half, b) if j == 1 else own(p2, 0, b, 1)
                        t.append(own(p0, half, b, j) + own(p1, 0, b, j) + final)
                above = jnp.where(row == 0, t[0], pltpu.roll(t[0], 1, 0))
                below = jnp.where(row == ROWS - 1, t[2], pltpu.roll(t[2], CELLS - 1, 0))
                for up, value in enumerate((above + t[1] + t[2], t[0] + t[1] + below)):
                    at = up * 2 * COLS + 2 * j + side
                    y_ref[pl.ds(at, CELLS, stride=4 * COLS), :] = value + bias
        o_ref[quarter ^ v] = y_ref[...].reshape(2 * CELLS, 2 * COLS, SLICE).astype(BF16)
        return 0

    lax.fori_loop(0, QUAD, combine, 0)


def spread_kernel(i_ref, o_ref, sem):
    copies = [
        pltpu.make_async_copy(i_ref.at[q], o_ref.at[:, :, pl.ds(q * SLICE, SLICE)], sem)
        for q in range(QUAD)
    ]
    for copy in copies:
        copy.start()
    for copy in copies:
        copy.wait()


def room(mebibytes):
    return pltpu.CompilerParams(vmem_limit_bytes=mebibytes * 2**20)


def vmem(n):
    return [pl.BlockSpec(memory_space=pltpu.VMEM)] * n


def shards(hidden, norm_gain, norm_shift, conv_weight, conv_bias):
    chips = lax.axis_size(CHIPS)
    share = 2 * conv_weight.shape[3]
    weight = conv_weight.reshape(TAPS, share // 2, CHANNELS)
    rows = lax.axis_size("zh")
    width = WIDE * CHANNELS + 128
    tiles = hidden.shape[0] // 8
    parcel, mine, row = pl.pallas_call(
        parcel_kernel,
        out_shape=(
            jax.ShapeDtypeStruct((tiles * CHANNELS // SLICE, 8, SLICE), BF16),
            jax.ShapeDtypeStruct((TAPS, share // 2, SLICE), BF16),
            jax.ShapeDtypeStruct((tiles, 8, CHANNELS), BF16),
        ),
        in_specs=[pl.BlockSpec(memory_space=pltpu.HBM)] * 2,
        out_specs=tuple(vmem(3)),
        scratch_shapes=[pltpu.SemaphoreType.DMA((2 + CHANNELS // SLICE,))],
        compiler_params=room(2),
        name="parcel",
    )(hidden.reshape(tiles, 8, CHANNELS), weight)
    parcel = lax.ppermute(parcel, "c", [(0, 1), (1, 0)])

    act_shape = (QUAD, WIDE, CELLS, CHANNELS)
    kin_shapes = tuple((n * rows, TAPS, share, SLICE) for n in (CLASSES - 1, 1))

    def blank(*shapes):
        return pl.pallas_call(
            lambda *refs: None,
            out_shape=tuple(jax.ShapeDtypeStruct(shape, BF16) for shape in shapes),
            out_specs=tuple(pl.BlockSpec(memory_space=pl.ANY) for _ in shapes),
            compiler_params=room(1),
            name="blank",
        )()

    def ring(step):
        return [(i, (i + step) % chips) for i in range(chips)]

    def activations(parcel, mine, row):
        packed = pl.pallas_call(
            pack_kernel,
            out_shape=jax.ShapeDtypeStruct((chips, 2, width), BF16),
            in_specs=vmem(2),
            out_specs=vmem(1)[0],
            compiler_params=room(6),
            name="pack",
        )(row, parcel)
        tiles = lax.all_to_all(packed, CHIPS, split_axis=0, concat_axis=0, tiled=True)
        active = pl.pallas_call(
            norm_kernel,
            out_shape=jax.ShapeDtypeStruct((WIDE, CELLS, CHANNELS), BF16),
            in_specs=vmem(3),
            out_specs=vmem(1)[0],
            compiler_params=room(6),
            name="norm",
        )(tiles, norm_gain[None], norm_shift[None])
        hops = [[(i, i ^ n) for i in range(QUAD)] for n in range(1, QUAD)]
        videos = [active] + [lax.ppermute(active, "gq", hop) for hop in hops]
        return (jnp.stack(videos),) + blank(*kin_shapes)

    def kernels(parcel, mine, row):
        mine = jnp.concatenate([parcel[:TAPS], mine], axis=1)
        kin = lax.all_gather(mine, "zh", axis=0)
        front, back = kin[: rows // 2], kin[rows // 2 :]
        below = [lax.ppermute(front, CHIPS, ring(1))]
        above = [lax.ppermute(back, CHIPS, ring(-1))]
        below += [lax.ppermute(back, CHIPS, ring(1))]
        above = [lax.ppermute(front, CHIPS, ring(-1))] + above
        low = lax.ppermute(below[0], CHIPS, ring(1))
        high = lax.ppermute(above[1], CHIPS, ring(-1))
        below, above = lax.optimization_barrier([jnp.concatenate(x) for x in (below, above)])
        near = jnp.concatenate([kin, below, above])
        return blank(act_shape) + (near, jnp.concatenate([low, high], axis=0))

    core = lax.axis_index("c")
    active, near, far = lax.cond(core == 0, activations, kernels, parcel, mine, row)
    right = [(2 * i, 2 * i + 2) for i in range(chips - 1)]
    left = [(j, i) for i, j in right]
    before = lax.ppermute(active[:, WIDE - 1], SPACE, right)
    after = lax.ppermute(active[:, 0], SPACE, left)
    given = lax.ppermute(active[:, 1:], "c", [(0, 1)])
    weights = (near, far)
    weights = tuple(lax.ppermute(w, "c", [(1, 0)]) for w in weights) + weights
    acts = (active, before, given, lax.ppermute(after, "c", [(0, 1)]))

    half = QUAD * CELLS
    out = pl.pallas_call(
        conv_kernel,
        out_shape=jax.ShapeDtypeStruct((QUAD, 2 * CELLS, 2 * COLS, SLICE), BF16),
        in_specs=vmem(5) + [pl.BlockSpec(memory_space=pltpu.HBM)] * 4,
        out_specs=vmem(1)[0],
        scratch_shapes=[
            pltpu.VMEM((TAPS, chips, share, SLICE), BF16),
            pltpu.VMEM((3, 4 * half, CHANNELS), BF16),
            pltpu.VMEM((3, 3 * half, SLICE), F32),
            pltpu.VMEM((3, 2 * half, SLICE), F32),
            pltpu.VMEM((3, 3 * half, SLICE), F32),
            pltpu.VMEM((4 * COLS * CELLS, SLICE), F32),
            pltpu.SemaphoreType.DMA,
        ],
        compiler_params=room(24),
        name="conv",
    )(*acts, conv_bias.astype(F32).reshape(QUAD, SLICE), *weights)
    out = lax.all_to_all(out, "gq", split_axis=0, concat_axis=0, tiled=True)
    out = pl.pallas_call(
        spread_kernel,
        out_shape=jax.ShapeDtypeStruct((2 * CELLS, 2 * COLS, CHANNELS), BF16),
        in_specs=vmem(1),
        out_specs=pl.BlockSpec(memory_space=pltpu.HBM),
        scratch_shapes=[pltpu.SemaphoreType.DMA],
        compiler_params=room(4),
        name="spread",
    )(out)
    return out.reshape(FRAMES, 2 * ROWS, 2 * COLS, CHANNELS)


def solution(mesh):
    groups, space = mesh.shape["groups"], mesh.shape["space"]
    torus = Mesh(
        mesh.devices.reshape(groups // QUAD, QUAD, space // (2 * CLASSES), CLASSES, 2),
        ("gh", "gq", "zh", "zl", "c"),
    )
    return jax.shard_map(
        shards,
        mesh=torus,
        in_specs=(
            P(("gh", "gq") + SPACE, None),
            P(),
            P(),
            P(None, None, None, SPACE, None),
            P(),
        ),
        out_specs=P(("gh", "gq"), None, SPACE, None),
        check_vma=False,
    )
```

```python
import functools

import jax
import jax.numpy as jnp
from jax import lax
from jax.experimental import pallas as pl
from jax.experimental.pallas import tpu as pltpu
from jax.sharding import Mesh
from jax.sharding import PartitionSpec as P

CHANNELS = 512
GROUPS = 32
FRAMES = 4
ROWS = 16
COLS = 2
WIDE = 2 * COLS
CLASSES = 4
CELLS = FRAMES * ROWS
MEMBERS = CHANNELS // GROUPS
QUAD = 4
SLICE = CHANNELS // QUAD
TAPS = 27
SPACE = ("zh", "zl", "c")
CHIPS = ("zh", "zl")
EPSILON = 1e-06
F32, BF16 = jnp.float32, jnp.bfloat16
HIGHEST = lax.Precision.HIGHEST


def iota(shape, dim):
    return lax.broadcasted_iota(jnp.int32, shape, dim)


def dot(a, b, precision=None):
    return jnp.dot(a, b, preferred_element_type=F32, precision=precision)


def in_pieces(v):
    high = v.astype(BF16)
    rest = v - high.astype(F32)
    middle = rest.astype(BF16)
    low = (rest - middle.astype(F32)).astype(BF16)
    lane = iota(v.shape, 1)
    return jnp.where(
        lane < GROUPS,
        high.astype(F32),
        jnp.where(lane < 2 * GROUPS, middle.astype(F32), low.astype(F32)),
    ).astype(BF16)


def parcel_kernel(x_ref, w_ref, g_ref, h_ref, p_ref, s_ref, r_ref, u_ref, v_ref, sem):
    core, quarter = lax.axis_index("c"), lax.axis_index("gq")
    lanes = pl.ds(pl.multiple_of(quarter * SLICE, SLICE), SLICE)
    tiles = x_ref.shape[0]

    def token_copies():
        return [
            pltpu.make_async_copy(
                x_ref.at[:, :, pl.ds(n * SLICE, SLICE)], p_ref.at[pl.ds(n * tiles, tiles)], sem.at[2 + n]
            )
            for n in range(CHANNELS // SLICE)
        ]

    def slice_copy():
        return pltpu.make_async_copy(w_ref.at[:, :, lanes], p_ref.at[pl.ds(0, TAPS)], sem.at[2])

    own = pltpu.make_async_copy(w_ref.at[:, :, lanes], s_ref, sem.at[0])
    row = pltpu.make_async_copy(x_ref, r_ref, sem.at[1])
    gain = pltpu.make_async_copy(g_ref, u_ref, sem.at[3])
    shift = pltpu.make_async_copy(h_ref, v_ref, sem.at[4])

    @pl.when(core == 0)
    def _():
        moves = (slice_copy(), row, gain, shift)
        for copy in moves:
            copy.start()
        for copy in moves:
            copy.wait()

    @pl.when(core == 1)
    def _():
        for copy in token_copies():
            copy.start()
        own.start()
        for copy in token_copies():
            copy.wait()
        own.wait()


def pack_kernel(x_ref, y_ref, o_ref):
    cells = x_ref.shape[0] * x_ref.shape[1]
    tiles = x_ref.shape[0]
    own = x_ref[...].astype(F32).reshape(cells, CHANNELS)
    given = [
        y_ref[n * tiles : (n + 1) * tiles].astype(F32).reshape(cells, SLICE)
        for n in range(CHANNELS // SLICE)
    ]
    rows = [own, jnp.concatenate(given, axis=1)]
    gather = jnp.where(
        (iota((CHANNELS, 128), 0) // MEMBERS == iota((CHANNELS, 128), 1) % GROUPS)
        & (iota((CHANNELS, 128), 1) < 3 * GROUPS),
        1.0,
        0.0,
    )
    spread = jnp.where(iota((128, CHANNELS), 0) == iota((128, CHANNELS), 1) // MEMBERS, 1.0, 0.0)

    def totals(values):
        return jnp.broadcast_to(sum(jnp.sum(v, axis=0, keepdims=True) for v in values), (8, CHANNELS))

    mean = dot(totals(rows), gather, HIGHEST) * (1.0 / (2 * cells * MEMBERS))
    away = [v - dot(mean, spread, HIGHEST)[:1] for v in rows]
    second = dot(totals([v * v for v in away]), gather, HIGHEST)
    stats = jnp.concatenate([in_pieces(mean)[:1], in_pieces(second)[:1]], axis=0)
    for d in range(cells // WIDE):
        for j in range(WIDE):
            c = d * WIDE + j
            pair = jnp.concatenate([v[c : c + 1] for v in rows], axis=0)
            o_ref[d, :, j * CHANNELS : (j + 1) * CHANNELS] = pair.astype(BF16)
        o_ref[d, :, WIDE * CHANNELS :] = stats


def norm_kernel(r_ref, gain_ref, shift_ref, o_ref):
    r = r_ref[...].astype(F32)
    sources = r.shape[0]

    def whole(v):
        return v + pltpu.roll(v, 128 - GROUPS, 1) + pltpu.roll(v, 128 - 2 * GROUPS, 1)

    means = whole(r[:, 0, WIDE * CHANNELS :])
    seconds = whole(r[:, 1, WIDE * CHANNELS :])
    each = float(2 * sources * WIDE * MEMBERS)
    mean = jnp.sum(means, axis=0, keepdims=True) * (1.0 / sources)
    second = jnp.sum(seconds, axis=0, keepdims=True) + each * jnp.sum(
        (means - mean) * (means - mean), axis=0, keepdims=True
    )
    real = iota((1, 128), 1) < GROUPS
    mean = jnp.where(real, mean, 0.0)
    scale = lax.rsqrt(jnp.where(real, second, 0.0) * (1.0 / (each * sources)) + EPSILON)
    spread = jnp.where(iota((128, CHANNELS), 0) == iota((128, CHANNELS), 1) // MEMBERS, 1.0, 0.0)
    mean = dot(jnp.broadcast_to(mean, (8, 128)), spread, HIGHEST)[:1]
    scale = dot(jnp.broadcast_to(scale, (8, 128)), spread, HIGHEST)[:1] * gain_ref[...]
    for j in range(WIDE):
        x = r[:, :, j * CHANNELS : (j + 1) * CHANNELS].reshape(2 * sources, CHANNELS)
        v = (x - mean) * scale + shift_ref[...]
        o_ref[j] = (v / (1.0 + jnp.exp(-v))).astype(BF16)


PASSES = (
    (((0, 0), (0, 1)), 0, 3),
    (((0, 2), (1, 0)), 0, 3),
    (((1, 1), (1, 2)), 1, 3),
    (((2, 0), (2, 1)), 1, 4),
    (((2, 2),), 1, 4),
)


def conv_kernel(videos, c_ref, w_ref, b_ref, *refs):
    outs, (x_ref, p0, p1, p2, y_ref) = refs[: len(videos)], refs[len(videos) :]
    core, kind, quarter = (lax.axis_index(n) for n in ("c", "zl", "gq"))
    place = lax.axis_index(CHIPS)
    final = lax.axis_size(CHIPS) - 1
    rows = w_ref.shape[0] // CLASSES
    count = len(videos)
    half = count * CELLS
    for n, v in enumerate(videos):
        block = [c_ref[v, j] for j in range(COLS + 2)]
        block[0] = jnp.where((core == 0) & (place == 0), block[1], block[0])
        block[3] = jnp.where((core == 1) & (place == final), block[2], block[3])
        for j in range(COLS + 2):
            for a in range(3):
                for f in range(FRAMES):
                    g = max(f + a - 2, 0)
                    start = j * half + n * CELLS + f * ROWS
                    x_ref[a, start : start + ROWS] = block[j][g * ROWS : (g + 1) * ROWS]

    lead = []
    for k in range(CLASSES):
        away = lax.rem(k + CLASSES - kind, CLASSES)
        lead.append(rows * jnp.where(away == 1, 2, jnp.where(away == 2, 3, jnp.where(away == 3, 1, 0))))

    def tap(t):
        return jnp.concatenate([w_ref[lead[k] + j, t] for j in range(rows) for k in range(CLASSES)], axis=0)

    store = (p0, p1, p2)
    offset = (0, 1, 1)
    for pair, lo, hi in PASSES:
        total = 0.0
        for a in range(3):
            w = [tap(a * 9 + b * 3 + e) for e, b in pair]
            w = jnp.concatenate(w, axis=1) if len(w) > 1 else w[0]
            total += dot(x_ref[a, lo * half : hi * half], w)
        for n, (e, b) in enumerate(pair):
            skip = (max(lo, offset[e]) - lo) * half
            store[e][b] = total[skip:, n * SLICE : (n + 1) * SLICE]

    bias = b_ref[pl.ds(quarter, 1)]
    row = iota((CELLS, SLICE), 0) % ROWS

    for n, o_ref in enumerate(outs):

        def part(e, b, j):
            start = (j - offset[e]) * half + n * CELLS
            return store[e][b, start : start + CELLS]

        for j in range(1, COLS + 1):
            for side in range(2):
                t = [
                    part(0, b, j - 1 + side) + part(1, b, j) + part(2, b, j + side) for b in range(3)
                ]
                above = jnp.where(row == 0, t[0], pltpu.roll(t[0], 1, 0))
                below = jnp.where(row == ROWS - 1, t[2], pltpu.roll(t[2], CELLS - 1, 0))
                for up, value in enumerate((above + t[1] + t[2], t[0] + t[1] + below)):
                    at = up * 2 * COLS + 2 * (j - 1) + side
                    y_ref[pl.ds(at, CELLS, stride=4 * COLS), :] = value + bias
        o_ref[...] = y_ref[...].reshape(2 * CELLS, 2 * COLS, SLICE).astype(BF16)


def convolve(videos, columns, weights, bias):
    half = len(videos) * CELLS
    return pl.pallas_call(
        functools.partial(conv_kernel, videos),
        out_shape=(jax.ShapeDtypeStruct((2 * CELLS, 2 * COLS, SLICE), BF16),) * len(videos),
        in_specs=vmem(3),
        out_specs=tuple(vmem(len(videos))),
        scratch_shapes=[
            pltpu.VMEM((3, 4 * half, CHANNELS), BF16),
            pltpu.VMEM((3, 3 * half, SLICE), F32),
            pltpu.VMEM((3, 2 * half, SLICE), F32),
            pltpu.VMEM((3, 3 * half, SLICE), F32),
            pltpu.VMEM((4 * COLS * CELLS, SLICE), F32),
        ],
        compiler_params=room(16),
        name="conv",
    )(columns, weights, bias)


def spread_kernel(*refs):
    o_ref, sem = refs[QUAD:]
    quarter = lax.axis_index("gq")
    copies = []
    for n in range(QUAD):
        lanes = pl.ds(pl.multiple_of((quarter ^ n) * SLICE, SLICE), SLICE)
        copies.append(pltpu.make_async_copy(refs[n], o_ref.at[:, :, lanes], sem.at[n]))
    for copy in copies:
        copy.start()
    for copy in copies:
        copy.wait()


def room(mebibytes):
    return pltpu.CompilerParams(vmem_limit_bytes=mebibytes * 2**20)


def vmem(n):
    return [pl.BlockSpec(memory_space=pltpu.VMEM)] * n


def shards(hidden, norm_gain, norm_shift, conv_weight, conv_bias):
    chips = lax.axis_size(CHIPS)
    share = 2 * conv_weight.shape[3]
    weight = conv_weight.reshape(TAPS, share // 2, CHANNELS)
    rows = lax.axis_size("zh")
    width = WIDE * CHANNELS + 128
    tiles = hidden.shape[0] // 8
    parcel, mine, row, gain, shift = pl.pallas_call(
        parcel_kernel,
        out_shape=(
            jax.ShapeDtypeStruct((tiles * CHANNELS // SLICE, 8, SLICE), BF16),
            jax.ShapeDtypeStruct((TAPS, share // 2, SLICE), BF16),
            jax.ShapeDtypeStruct((tiles, 8, CHANNELS), BF16),
            jax.ShapeDtypeStruct((1, CHANNELS), F32),
            jax.ShapeDtypeStruct((1, CHANNELS), F32),
        ),
        in_specs=[pl.BlockSpec(memory_space=pltpu.HBM)] * 4,
        out_specs=tuple(vmem(5)),
        scratch_shapes=[pltpu.SemaphoreType.DMA((2 + CHANNELS // SLICE,))],
        compiler_params=pltpu.CompilerParams(vmem_limit_bytes=66563328),
        name="parcel",
    )(hidden.reshape(tiles, 8, CHANNELS), weight, norm_gain[None], norm_shift[None])
    parcel = lax.ppermute(parcel, "c", [(0, 1), (1, 0)])

    act_shape = (QUAD, WIDE, CELLS, CHANNELS)
    kin_shape = (CLASSES * rows, TAPS, share, SLICE)

    def blank(*shapes):
        return pl.pallas_call(
            lambda *refs: None,
            out_shape=tuple(jax.ShapeDtypeStruct(shape, BF16) for shape in shapes),
            out_specs=tuple(pl.BlockSpec(memory_space=pl.ANY) for _ in shapes),
            compiler_params=room(1),
            name="blank",
        )()

    def ring(step):
        return [(i, (i + step) % chips) for i in range(chips)]

    def activations(parcel, mine, row, gain, shift):
        packed = pl.pallas_call(
            pack_kernel,
            out_shape=jax.ShapeDtypeStruct((chips, 2, width), BF16),
            in_specs=vmem(2),
            out_specs=vmem(1)[0],
            compiler_params=room(6),
            name="pack",
        )(row, parcel)
        tiles = lax.all_to_all(packed, CHIPS, split_axis=0, concat_axis=0, tiled=True)
        active = pl.pallas_call(
            norm_kernel,
            out_shape=jax.ShapeDtypeStruct((WIDE, CELLS, CHANNELS), BF16),
            in_specs=vmem(3),
            out_specs=vmem(1)[0],
            compiler_params=room(6),
            name="norm",
        )(tiles, gain, shift)
        hops = [[(i, i ^ n) for i in range(QUAD)] for n in range(1, QUAD)]
        videos = [active] + [lax.ppermute(active, "gq", hop) for hop in hops]
        return (jnp.stack(videos),) + blank(kin_shape)

    def kernels(parcel, mine, row, gain, shift):
        mine = jnp.concatenate([parcel[:TAPS], mine], axis=1)
        kin = lax.all_gather(mine, "zh", axis=0)
        front, back = kin[: rows // 2], kin[rows // 2 :]
        below = [lax.ppermute(front, CHIPS, ring(1))]
        above = [lax.ppermute(back, CHIPS, ring(-1))]
        below += [lax.ppermute(back, CHIPS, ring(1))]
        above = [lax.ppermute(front, CHIPS, ring(-1))] + above
        low = lax.ppermute(below[0], CHIPS, ring(1))
        high = lax.ppermute(above[1], CHIPS, ring(-1))
        below, above = lax.optimization_barrier([jnp.concatenate(x) for x in (below, above)])
        near = jnp.concatenate([kin, below, above])
        far = jnp.concatenate([low, high])
        near, far = lax.optimization_barrier((near, far))
        return blank(act_shape) + (jnp.concatenate([near, far]),)

    core = lax.axis_index("c")
    active, weights = lax.cond(core == 0, activations, kernels, parcel, mine, row, gain, shift)
    right = [(2 * i, 2 * i + 2) for i in range(chips - 1)]
    left = [(j, i) for i, j in right]
    before = lax.ppermute(active[:, WIDE - 1], SPACE, right)
    after = lax.ppermute(active[:, 0], SPACE, left)
    brought = lax.ppermute(weights, "c", [(1, 0)])
    given = lax.ppermute(jnp.concatenate([active[:, 1:], after[:, None]], axis=1), "c", [(0, 1)])
    columns = jnp.concatenate([before[:, None], active[:, :WIDE - 1]], axis=1)
    bias = conv_bias.astype(F32).reshape(QUAD, SLICE)

    columns = jnp.where(core == 0, columns, given)
    weights = jnp.where(core == 0, brought, weights)
    outs = list(convolve(tuple(range(QUAD)), columns, weights, bias))
    for n in range(1, QUAD):
        outs[n] = lax.ppermute(outs[n], "gq", [(i, i ^ n) for i in range(QUAD)])
    out = pl.pallas_call(
        spread_kernel,
        out_shape=jax.ShapeDtypeStruct((2 * CELLS, 2 * COLS, CHANNELS), BF16),
        in_specs=vmem(QUAD),
        out_specs=pl.BlockSpec(memory_space=pltpu.HBM),
        scratch_shapes=[pltpu.SemaphoreType.DMA((QUAD,))],
        compiler_params=room(4),
        name="spread",
    )(*outs)
    return out.reshape(FRAMES, 2 * ROWS, 2 * COLS, CHANNELS)


def solution(mesh):
    groups, space = mesh.shape["groups"], mesh.shape["space"]
    torus = Mesh(
        mesh.devices.reshape(groups // QUAD, QUAD, space // (2 * CLASSES), CLASSES, 2),
        ("gh", "gq", "zh", "zl", "c"),
    )
    return jax.shard_map(
        shards,
        mesh=torus,
        in_specs=(
            P(("gh", "gq") + SPACE, None),
            P(),
            P(),
            P(None, None, None, SPACE, None),
            P(),
        ),
        out_specs=P(("gh", "gq"), None, SPACE, None),
        check_vma=False,
    )
```

```python
import functools

import jax
import jax.numpy as jnp
from jax import lax
from jax.experimental import pallas as pl
from jax.experimental.pallas import tpu as pltpu
from jax.sharding import Mesh
from jax.sharding import PartitionSpec as P

CHANNELS = 512
GROUPS = 32
FRAMES = 4
ROWS = 16
COLS = 2
WIDE = 2 * COLS
CLASSES = 4
CELLS = FRAMES * ROWS
MEMBERS = CHANNELS // GROUPS
QUAD = 4
SLICE = CHANNELS // QUAD
TAPS = 27
SPACE = ("zh", "zl", "c")
CHIPS = ("zh", "zl")
EPSILON = 1e-06
F32, BF16 = jnp.float32, jnp.bfloat16
HIGHEST = lax.Precision.HIGHEST


def iota(shape, dim):
    return lax.broadcasted_iota(jnp.int32, shape, dim)


def dot(a, b, precision=None):
    return jnp.dot(a, b, preferred_element_type=F32, precision=precision)


def in_pieces(v):
    high = v.astype(BF16)
    rest = v - high.astype(F32)
    middle = rest.astype(BF16)
    low = (rest - middle.astype(F32)).astype(BF16)
    lane = iota(v.shape, 1)
    return jnp.where(
        lane < GROUPS,
        high.astype(F32),
        jnp.where(lane < 2 * GROUPS, middle.astype(F32), low.astype(F32)),
    ).astype(BF16)


def parcel_kernel(x_ref, w_ref, g_ref, h_ref, p_ref, s_ref, r_ref, u_ref, v_ref, sem):
    core, quarter = lax.axis_index("c"), lax.axis_index("gq")
    lanes = pl.ds(pl.multiple_of(quarter * SLICE, SLICE), SLICE)
    tiles = x_ref.shape[0]

    def token_copies():
        return [
            pltpu.make_async_copy(
                x_ref.at[:, :, pl.ds(n * SLICE, SLICE)], p_ref.at[pl.ds(n * tiles, tiles)], sem.at[2 + n]
            )
            for n in range(CHANNELS // SLICE)
        ]

    def slice_copy():
        return pltpu.make_async_copy(w_ref.at[:, :, lanes], p_ref.at[pl.ds(0, TAPS)], sem.at[2])

    own = pltpu.make_async_copy(w_ref.at[:, :, lanes], s_ref, sem.at[0])
    row = pltpu.make_async_copy(x_ref, r_ref, sem.at[1])
    gain = pltpu.make_async_copy(g_ref, u_ref, sem.at[3])
    shift = pltpu.make_async_copy(h_ref, v_ref, sem.at[4])

    @pl.when(core == 0)
    def _():
        moves = (slice_copy(), row, gain, shift)
        for copy in moves:
            copy.start()
        for copy in moves:
            copy.wait()

    @pl.when(core == 1)
    def _():
        for copy in token_copies():
            copy.start()
        own.start()
        for copy in token_copies():
            copy.wait()
        own.wait()


def pack_kernel(x_ref, y_ref, o_ref):
    cells = x_ref.shape[0] * x_ref.shape[1]
    tiles = x_ref.shape[0]
    own = x_ref[...].astype(F32).reshape(cells, CHANNELS)
    given = [
        y_ref[n * tiles : (n + 1) * tiles].astype(F32).reshape(cells, SLICE)
        for n in range(CHANNELS // SLICE)
    ]
    rows = [own, jnp.concatenate(given, axis=1)]
    gather = jnp.where(
        (iota((CHANNELS, 128), 0) // MEMBERS == iota((CHANNELS, 128), 1) % GROUPS)
        & (iota((CHANNELS, 128), 1) < 3 * GROUPS),
        1.0,
        0.0,
    )
    spread = jnp.where(iota((128, CHANNELS), 0) == iota((128, CHANNELS), 1) // MEMBERS, 1.0, 0.0)

    def totals(values):
        return jnp.broadcast_to(sum(jnp.sum(v, axis=0, keepdims=True) for v in values), (8, CHANNELS))

    mean = dot(totals(rows), gather, HIGHEST) * (1.0 / (2 * cells * MEMBERS))
    away = [v - dot(mean, spread, HIGHEST)[:1] for v in rows]
    second = dot(totals([v * v for v in away]), gather, HIGHEST)
    stats = jnp.concatenate([in_pieces(mean)[:1], in_pieces(second)[:1]], axis=0)
    for d in range(cells // WIDE):
        for j in range(WIDE):
            c = d * WIDE + j
            pair = jnp.concatenate([v[c : c + 1] for v in rows], axis=0)
            o_ref[d, :, j * CHANNELS : (j + 1) * CHANNELS] = pair.astype(BF16)
        o_ref[d, :, WIDE * CHANNELS :] = stats


def norm_kernel(r_ref, gain_ref, shift_ref, o_ref):
    r = r_ref[...].astype(F32)
    sources = r.shape[0]

    def whole(v):
        return v + pltpu.roll(v, 128 - GROUPS, 1) + pltpu.roll(v, 128 - 2 * GROUPS, 1)

    means = whole(r[:, 0, WIDE * CHANNELS :])
    seconds = whole(r[:, 1, WIDE * CHANNELS :])
    each = float(2 * sources * WIDE * MEMBERS)
    mean = jnp.sum(means, axis=0, keepdims=True) * (1.0 / sources)
    second = jnp.sum(seconds, axis=0, keepdims=True) + each * jnp.sum(
        (means - mean) * (means - mean), axis=0, keepdims=True
    )
    real = iota((1, 128), 1) < GROUPS
    mean = jnp.where(real, mean, 0.0)
    scale = lax.rsqrt(jnp.where(real, second, 0.0) * (1.0 / (each * sources)) + EPSILON)
    spread = jnp.where(iota((128, CHANNELS), 0) == iota((128, CHANNELS), 1) // MEMBERS, 1.0, 0.0)
    mean = dot(jnp.broadcast_to(mean, (8, 128)), spread, HIGHEST)[:1]
    scale = dot(jnp.broadcast_to(scale, (8, 128)), spread, HIGHEST)[:1] * gain_ref[...]
    for j in range(WIDE):
        x = r[:, :, j * CHANNELS : (j + 1) * CHANNELS].reshape(2 * sources, CHANNELS)
        v = (x - mean) * scale + shift_ref[...]
        o_ref[j] = (v / (1.0 + jnp.exp(-v))).astype(BF16)


PASSES = (
    (((0, 0), (0, 1)), 0, 3),
    (((0, 2), (1, 0)), 0, 3),
    (((1, 1), (1, 2)), 1, 3),
    (((2, 0), (2, 1)), 1, 4),
    (((2, 2),), 1, 4),
)


def conv_kernel(videos, c_ref, w_ref, b_ref, *refs):
    outs, (x_ref, p0, p1, p2, y_ref) = refs[: len(videos)], refs[len(videos) :]
    core, kind, quarter = (lax.axis_index(n) for n in ("c", "zl", "gq"))
    place = lax.axis_index(CHIPS)
    final = lax.axis_size(CHIPS) - 1
    rows = w_ref.shape[0] // CLASSES
    count = len(videos)
    half = count * CELLS
    for n, v in enumerate(videos):
        block = [c_ref[v, j] for j in range(COLS + 2)]
        block[0] = jnp.where((core == 0) & (place == 0), block[1], block[0])
        block[3] = jnp.where((core == 1) & (place == final), block[2], block[3])
        for j in range(COLS + 2):
            for a in range(3):
                for f in range(FRAMES):
                    g = max(f + a - 2, 0)
                    start = j * half + n * CELLS + f * ROWS
                    x_ref[a, start : start + ROWS] = block[j][g * ROWS : (g + 1) * ROWS]

    lead = []
    for k in range(CLASSES):
        away = lax.rem(k + CLASSES - kind, CLASSES)
        lead.append(rows * jnp.where(away == 1, 2, jnp.where(away == 2, 3, jnp.where(away == 3, 1, 0))))

    def tap(t):
        return jnp.concatenate([w_ref[lead[k] + j, t] for j in range(rows) for k in range(CLASSES)], axis=0)

    store = (p0, p1, p2)
    offset = (0, 1, 1)
    for pair, lo, hi in PASSES:
        total = 0.0
        for a in range(3):
            w = [tap(a * 9 + b * 3 + e) for e, b in pair]
            w = jnp.concatenate(w, axis=1) if len(w) > 1 else w[0]
            total += dot(x_ref[a, lo * half : hi * half], w)
        for n, (e, b) in enumerate(pair):
            skip = (max(lo, offset[e]) - lo) * half
            store[e][b] = total[skip:, n * SLICE : (n + 1) * SLICE]

    bias = b_ref[pl.ds(quarter, 1)]
    row = iota((CELLS, SLICE), 0) % ROWS

    for n, o_ref in enumerate(outs):

        def part(e, b, j):
            start = (j - offset[e]) * half + n * CELLS
            return store[e][b, start : start + CELLS]

        for j in range(1, COLS + 1):
            for side in range(2):
                t = [
                    part(0, b, j - 1 + side) + part(1, b, j) + part(2, b, j + side) for b in range(3)
                ]
                above = jnp.where(row == 0, t[0], pltpu.roll(t[0], 1, 0))
                below = jnp.where(row == ROWS - 1, t[2], pltpu.roll(t[2], CELLS - 1, 0))
                for up, value in enumerate((above + t[1] + t[2], t[0] + t[1] + below)):
                    at = up * 2 * COLS + 2 * (j - 1) + side
                    y_ref[pl.ds(at, CELLS, stride=4 * COLS), :] = value + bias
        o_ref[...] = y_ref[...].reshape(2 * CELLS, 2 * COLS, SLICE).astype(BF16)


def convolve(videos, columns, weights, bias):
    half = len(videos) * CELLS
    return pl.pallas_call(
        functools.partial(conv_kernel, videos),
        out_shape=(jax.ShapeDtypeStruct((2 * CELLS, 2 * COLS, SLICE), BF16),) * len(videos),
        in_specs=vmem(3),
        out_specs=tuple(vmem(len(videos))),
        scratch_shapes=[
            pltpu.VMEM((3, 4 * half, CHANNELS), BF16),
            pltpu.VMEM((3, 3 * half, SLICE), F32),
            pltpu.VMEM((3, 2 * half, SLICE), F32),
            pltpu.VMEM((3, 3 * half, SLICE), F32),
            pltpu.VMEM((4 * COLS * CELLS, SLICE), F32),
        ],
        compiler_params=room(16),
        name="conv",
    )(columns, weights, bias)


def spread_kernel(*refs):
    o_ref, sem = refs[QUAD:]
    quarter = lax.axis_index("gq")
    copies = []
    for n in range(QUAD):
        lanes = pl.ds(pl.multiple_of((quarter ^ n) * SLICE, SLICE), SLICE)
        copies.append(pltpu.make_async_copy(refs[n], o_ref.at[:, :, lanes], sem.at[n]))
    for copy in copies:
        copy.start()
    for copy in copies:
        copy.wait()


def room(mebibytes):
    return pltpu.CompilerParams(vmem_limit_bytes=mebibytes * 2**20)


def vmem(n):
    return [pl.BlockSpec(memory_space=pltpu.VMEM)] * n


def shards(hidden, norm_gain, norm_shift, conv_weight, conv_bias):
    chips = lax.axis_size(CHIPS)
    share = 2 * conv_weight.shape[3]
    weight = conv_weight.reshape(TAPS, share // 2, CHANNELS)
    rows = lax.axis_size("zh")
    width = WIDE * CHANNELS + 128
    tiles = hidden.shape[0] // 8
    parcel, mine, row, gain, shift = pl.pallas_call(
        parcel_kernel,
        out_shape=(
            jax.ShapeDtypeStruct((tiles * CHANNELS // SLICE, 8, SLICE), BF16),
            jax.ShapeDtypeStruct((TAPS, share // 2, SLICE), BF16),
            jax.ShapeDtypeStruct((tiles, 8, CHANNELS), BF16),
            jax.ShapeDtypeStruct((1, CHANNELS), F32),
            jax.ShapeDtypeStruct((1, CHANNELS), F32),
        ),
        in_specs=[pl.BlockSpec(memory_space=pltpu.HBM)] * 4,
        out_specs=tuple(vmem(5)),
        scratch_shapes=[pltpu.SemaphoreType.DMA((2 + CHANNELS // SLICE,))],
        compiler_params=pltpu.CompilerParams(vmem_limit_bytes=66563328),
        name="parcel",
    )(hidden.reshape(tiles, 8, CHANNELS), weight, norm_gain[None], norm_shift[None])
    parcel = lax.ppermute(parcel, "c", [(0, 1), (1, 0)])

    act_shape = (QUAD, WIDE, CELLS, CHANNELS)
    kin_shape = (CLASSES * rows, TAPS, share, SLICE)

    def blank(*shapes):
        return pl.pallas_call(
            lambda *refs: None,
            out_shape=tuple(jax.ShapeDtypeStruct(shape, BF16) for shape in shapes),
            out_specs=tuple(pl.BlockSpec(memory_space=pl.ANY) for _ in shapes),
            compiler_params=room(1),
            name="blank",
        )()

    def ring(step):
        return [(i, (i + step) % chips) for i in range(chips)]

    def activations(parcel, mine, row, gain, shift):
        packed = pl.pallas_call(
            pack_kernel,
            out_shape=jax.ShapeDtypeStruct((chips, 2, width), BF16),
            in_specs=vmem(2),
            out_specs=vmem(1)[0],
            compiler_params=room(6),
            name="pack",
        )(row, parcel)
        tiles = lax.all_to_all(packed, CHIPS, split_axis=0, concat_axis=0, tiled=True)
        active = pl.pallas_call(
            norm_kernel,
            out_shape=jax.ShapeDtypeStruct((WIDE, CELLS, CHANNELS), BF16),
            in_specs=vmem(3),
            out_specs=vmem(1)[0],
            compiler_params=room(6),
            name="norm",
        )(tiles, gain, shift)
        hops = [[(i, i ^ n) for i in range(QUAD)] for n in range(1, QUAD)]
        videos = [active] + [lax.ppermute(active, "gq", hop) for hop in hops]
        return (jnp.stack(videos),) + blank(kin_shape)

    def kernels(parcel, mine, row, gain, shift):
        mine = jnp.concatenate([parcel[:TAPS], mine], axis=1)
        kin = lax.all_gather(mine, "zh", axis=0)
        front, back = kin[: rows // 2], kin[rows // 2 :]
        below = [lax.ppermute(front, CHIPS, ring(1))]
        above = [lax.ppermute(back, CHIPS, ring(-1))]
        below += [lax.ppermute(back, CHIPS, ring(1))]
        above = [lax.ppermute(front, CHIPS, ring(-1))] + above
        low = lax.ppermute(below[0], CHIPS, ring(1))
        high = lax.ppermute(above[1], CHIPS, ring(-1))
        below, above = lax.optimization_barrier([jnp.concatenate(x) for x in (below, above)])
        near = jnp.concatenate([kin, below, above])
        far = jnp.concatenate([low, high])
        near, far = lax.optimization_barrier((near, far))
        return blank(act_shape) + (jnp.concatenate([near, far]),)

    core = lax.axis_index("c")
    active, weights = lax.cond(core == 0, activations, kernels, parcel, mine, row, gain, shift)
    right = [(2 * i, 2 * i + 2) for i in range(chips - 1)]
    left = [(j, i) for i, j in right]
    before = lax.ppermute(active[:, WIDE - 1], SPACE, right)
    after = lax.ppermute(active[:, 0], SPACE, left)
    brought = lax.ppermute(weights, "c", [(1, 0)])
    given = lax.ppermute(jnp.concatenate([active[:, 1:], after[:, None]], axis=1), "c", [(0, 1)])
    columns = jnp.concatenate([before[:, None], active[:, :WIDE - 1]], axis=1)
    bias = conv_bias.astype(F32).reshape(QUAD, SLICE)

    columns = jnp.where(core == 0, columns, given)
    weights = jnp.where(core == 0, brought, weights)
    outs = [None] * QUAD
    for n in reversed(range(QUAD)):
        outs[n] = convolve((n,), columns, weights, bias)[0]
        if n:
            outs[n] = lax.ppermute(outs[n], "gq", [(i, i ^ n) for i in range(QUAD)])
    out = pl.pallas_call(
        spread_kernel,
        out_shape=jax.ShapeDtypeStruct((2 * CELLS, 2 * COLS, CHANNELS), BF16),
        in_specs=vmem(QUAD),
        out_specs=pl.BlockSpec(memory_space=pltpu.HBM),
        scratch_shapes=[pltpu.SemaphoreType.DMA((QUAD,))],
        compiler_params=room(4),
        name="spread",
    )(*outs)
    return out.reshape(FRAMES, 2 * ROWS, 2 * COLS, CHANNELS)


def solution(mesh):
    groups, space = mesh.shape["groups"], mesh.shape["space"]
    torus = Mesh(
        mesh.devices.reshape(groups // QUAD, QUAD, space // (2 * CLASSES), CLASSES, 2),
        ("gh", "gq", "zh", "zl", "c"),
    )
    return jax.shard_map(
        shards,
        mesh=torus,
        in_specs=(
            P(("gh", "gq") + SPACE, None),
            P(),
            P(),
            P(None, None, None, SPACE, None),
            P(),
        ),
        out_specs=P(("gh", "gq"), None, SPACE, None),
        check_vma=False,
    )
```

```python
import functools

import jax
import jax.numpy as jnp
from jax import lax
from jax.experimental import pallas as pl
from jax.experimental.pallas import tpu as pltpu
from jax.sharding import Mesh
from jax.sharding import PartitionSpec as P

CHANNELS = 512
GROUPS = 32
FRAMES = 4
ROWS = 16
COLS = 2
WIDE = 2 * COLS
CLASSES = 4
CELLS = FRAMES * ROWS
MEMBERS = CHANNELS // GROUPS
QUAD = 4
SLICE = CHANNELS // QUAD
TAPS = 27
SPACE = ("zh", "zl", "c")
CHIPS = ("zh", "zl")
EPSILON = 1e-06
F32, BF16 = jnp.float32, jnp.bfloat16
HIGHEST = lax.Precision.HIGHEST


def iota(shape, dim):
    return lax.broadcasted_iota(jnp.int32, shape, dim)


def dot(a, b, precision=None):
    return jnp.dot(a, b, preferred_element_type=F32, precision=precision)


def in_pieces(v):
    high = v.astype(BF16)
    rest = v - high.astype(F32)
    middle = rest.astype(BF16)
    low = (rest - middle.astype(F32)).astype(BF16)
    lane = iota(v.shape, 1)
    return jnp.where(
        lane < GROUPS,
        high.astype(F32),
        jnp.where(lane < 2 * GROUPS, middle.astype(F32), low.astype(F32)),
    ).astype(BF16)


def parcel_kernel(x_ref, w_ref, g_ref, h_ref, p_ref, s_ref, r_ref, u_ref, v_ref, sem):
    core, quarter = lax.axis_index("c"), lax.axis_index("gq")
    lanes = pl.ds(pl.multiple_of(quarter * SLICE, SLICE), SLICE)
    tiles = x_ref.shape[0]

    def token_copies():
        return [
            pltpu.make_async_copy(
                x_ref.at[:, :, pl.ds(n * SLICE, SLICE)], p_ref.at[pl.ds(n * tiles, tiles)], sem.at[2 + n]
            )
            for n in range(CHANNELS // SLICE)
        ]

    def slice_copy():
        return pltpu.make_async_copy(w_ref.at[:, :, lanes], p_ref.at[pl.ds(0, TAPS)], sem.at[2])

    own = pltpu.make_async_copy(w_ref.at[:, :, lanes], s_ref, sem.at[0])
    row = pltpu.make_async_copy(x_ref, r_ref, sem.at[1])
    gain = pltpu.make_async_copy(g_ref, u_ref, sem.at[3])
    shift = pltpu.make_async_copy(h_ref, v_ref, sem.at[4])

    @pl.when(core == 0)
    def _():
        moves = (slice_copy(), row, gain, shift)
        for copy in moves:
            copy.start()
        for copy in moves:
            copy.wait()

    @pl.when(core == 1)
    def _():
        for copy in token_copies():
            copy.start()
        own.start()
        for copy in token_copies():
            copy.wait()
        own.wait()


def pack_kernel(x_ref, y_ref, o_ref):
    cells = x_ref.shape[0] * x_ref.shape[1]
    tiles = x_ref.shape[0]
    own = x_ref[...].astype(F32).reshape(cells, CHANNELS)
    given = [
        y_ref[n * tiles : (n + 1) * tiles].astype(F32).reshape(cells, SLICE)
        for n in range(CHANNELS // SLICE)
    ]
    rows = [own, jnp.concatenate(given, axis=1)]
    gather = jnp.where(
        (iota((CHANNELS, 128), 0) // MEMBERS == iota((CHANNELS, 128), 1) % GROUPS)
        & (iota((CHANNELS, 128), 1) < 3 * GROUPS),
        1.0,
        0.0,
    )
    spread = jnp.where(iota((128, CHANNELS), 0) == iota((128, CHANNELS), 1) // MEMBERS, 1.0, 0.0)

    def totals(values):
        return jnp.broadcast_to(sum(jnp.sum(v, axis=0, keepdims=True) for v in values), (8, CHANNELS))

    mean = dot(totals(rows), gather, HIGHEST) * (1.0 / (2 * cells * MEMBERS))
    away = [v - dot(mean, spread, HIGHEST)[:1] for v in rows]
    second = dot(totals([v * v for v in away]), gather, HIGHEST)
    stats = jnp.concatenate([in_pieces(mean)[:1], in_pieces(second)[:1]], axis=0)
    for d in range(cells // WIDE):
        for j in range(WIDE):
            c = d * WIDE + j
            pair = jnp.concatenate([v[c : c + 1] for v in rows], axis=0)
            o_ref[d, :, j * CHANNELS : (j + 1) * CHANNELS] = pair.astype(BF16)
        o_ref[d, :, WIDE * CHANNELS :] = stats


def norm_kernel(r_ref, gain_ref, shift_ref, o_ref):
    r = r_ref[...].astype(F32)
    sources = r.shape[0]

    def whole(v):
        return v + pltpu.roll(v, 128 - GROUPS, 1) + pltpu.roll(v, 128 - 2 * GROUPS, 1)

    means = whole(r[:, 0, WIDE * CHANNELS :])
    seconds = whole(r[:, 1, WIDE * CHANNELS :])
    each = float(2 * sources * WIDE * MEMBERS)
    mean = jnp.sum(means, axis=0, keepdims=True) * (1.0 / sources)
    second = jnp.sum(seconds, axis=0, keepdims=True) + each * jnp.sum(
        (means - mean) * (means - mean), axis=0, keepdims=True
    )
    real = iota((1, 128), 1) < GROUPS
    mean = jnp.where(real, mean, 0.0)
    scale = lax.rsqrt(jnp.where(real, second, 0.0) * (1.0 / (each * sources)) + EPSILON)
    spread = jnp.where(iota((128, CHANNELS), 0) == iota((128, CHANNELS), 1) // MEMBERS, 1.0, 0.0)
    mean = dot(jnp.broadcast_to(mean, (8, 128)), spread, HIGHEST)[:1]
    scale = dot(jnp.broadcast_to(scale, (8, 128)), spread, HIGHEST)[:1] * gain_ref[...]
    for j in range(WIDE):
        x = r[:, :, j * CHANNELS : (j + 1) * CHANNELS].reshape(2 * sources, CHANNELS)
        v = (x - mean) * scale + shift_ref[...]
        o_ref[j] = (v / (1.0 + jnp.exp(-v))).astype(BF16)


PASSES = (
    (((0, 0), (0, 1)), 0, 3),
    (((0, 2), (1, 0)), 0, 3),
    (((1, 1), (1, 2)), 1, 3),
    (((2, 0), (2, 1)), 1, 4),
    (((2, 2),), 1, 4),
)


def conv_kernel(videos, c_ref, w_ref, b_ref, *refs):
    outs, (x_ref, p0, p1, p2, y_ref) = refs[: len(videos)], refs[len(videos) :]
    core, kind, quarter = (lax.axis_index(n) for n in ("c", "zl", "gq"))
    place = lax.axis_index(CHIPS)
    final = lax.axis_size(CHIPS) - 1
    rows = w_ref.shape[0] // CLASSES
    count = len(videos)
    half = count * CELLS
    for n, v in enumerate(videos):
        block = [c_ref[v, j] for j in range(COLS + 2)]
        block[0] = jnp.where((core == 0) & (place == 0), block[1], block[0])
        block[3] = jnp.where((core == 1) & (place == final), block[2], block[3])
        for j in range(COLS + 2):
            for a in range(3):
                for f in range(FRAMES):
                    g = max(f + a - 2, 0)
                    start = j * half + n * CELLS + f * ROWS
                    x_ref[a, start : start + ROWS] = block[j][g * ROWS : (g + 1) * ROWS]

    lead = []
    for k in range(CLASSES):
        away = lax.rem(k + CLASSES - kind, CLASSES)
        lead.append(rows * jnp.where(away == 1, 2, jnp.where(away == 2, 3, jnp.where(away == 3, 1, 0))))

    def tap(t):
        return jnp.concatenate([w_ref[lead[k] + j, t] for j in range(rows) for k in range(CLASSES)], axis=0)

    store = (p0, p1, p2)
    offset = (0, 1, 1)
    for pair, lo, hi in PASSES:
        total = 0.0
        for a in range(3):
            w = [tap(a * 9 + b * 3 + e) for e, b in pair]
            w = jnp.concatenate(w, axis=1) if len(w) > 1 else w[0]
            total += dot(x_ref[a, lo * half : hi * half], w)
        for n, (e, b) in enumerate(pair):
            skip = (max(lo, offset[e]) - lo) * half
            store[e][b] = total[skip:, n * SLICE : (n + 1) * SLICE]

    bias = b_ref[pl.ds(quarter, 1)]
    row = iota((CELLS, SLICE), 0) % ROWS

    for n, o_ref in enumerate(outs):

        def part(e, b, j):
            start = (j - offset[e]) * half + n * CELLS
            return store[e][b, start : start + CELLS]

        for j in range(1, COLS + 1):
            for side in range(2):
                t = [
                    part(0, b, j - 1 + side) + part(1, b, j) + part(2, b, j + side) for b in range(3)
                ]
                above = jnp.where(row == 0, t[0], pltpu.roll(t[0], 1, 0))
                below = jnp.where(row == ROWS - 1, t[2], pltpu.roll(t[2], CELLS - 1, 0))
                for up, value in enumerate((above + t[1] + t[2], t[0] + t[1] + below)):
                    at = up * 2 * COLS + 2 * (j - 1) + side
                    y_ref[pl.ds(at, CELLS, stride=4 * COLS), :] = value + bias
        o_ref[...] = y_ref[...].reshape(2 * CELLS, 2 * COLS, SLICE).astype(BF16)


def convolve(videos, columns, weights, bias):
    half = len(videos) * CELLS
    return pl.pallas_call(
        functools.partial(conv_kernel, videos),
        out_shape=(jax.ShapeDtypeStruct((2 * CELLS, 2 * COLS, SLICE), BF16),) * len(videos),
        in_specs=vmem(3),
        out_specs=tuple(vmem(len(videos))),
        scratch_shapes=[
            pltpu.VMEM((3, 4 * half, CHANNELS), BF16),
            pltpu.VMEM((3, 3 * half, SLICE), F32),
            pltpu.VMEM((3, 2 * half, SLICE), F32),
            pltpu.VMEM((3, 3 * half, SLICE), F32),
            pltpu.VMEM((4 * COLS * CELLS, SLICE), F32),
        ],
        compiler_params=room(16),
        name="conv",
    )(columns, weights, bias)


def spread_kernel(*refs):
    o_ref, sem = refs[QUAD:]
    quarter = lax.axis_index("gq")
    copies = []
    for n in range(QUAD):
        lanes = pl.ds(pl.multiple_of((quarter ^ n) * SLICE, SLICE), SLICE)
        copies.append(pltpu.make_async_copy(refs[n], o_ref.at[:, :, lanes], sem.at[n]))
    for copy in copies:
        copy.start()
    for copy in copies:
        copy.wait()


def room(mebibytes):
    return pltpu.CompilerParams(vmem_limit_bytes=mebibytes * 2**20)


def vmem(n):
    return [pl.BlockSpec(memory_space=pltpu.VMEM)] * n


def shards(hidden, norm_gain, norm_shift, conv_weight, conv_bias):
    chips = lax.axis_size(CHIPS)
    share = 2 * conv_weight.shape[3]
    weight = conv_weight.reshape(TAPS, share // 2, CHANNELS)
    rows = lax.axis_size("zh")
    width = WIDE * CHANNELS + 128
    tiles = hidden.shape[0] // 8
    parcel, mine, row, gain, shift = pl.pallas_call(
        parcel_kernel,
        out_shape=(
            jax.ShapeDtypeStruct((tiles * CHANNELS // SLICE, 8, SLICE), BF16),
            jax.ShapeDtypeStruct((TAPS, share // 2, SLICE), BF16),
            jax.ShapeDtypeStruct((tiles, 8, CHANNELS), BF16),
            jax.ShapeDtypeStruct((1, CHANNELS), F32),
            jax.ShapeDtypeStruct((1, CHANNELS), F32),
        ),
        in_specs=[pl.BlockSpec(memory_space=pltpu.HBM)] * 4,
        out_specs=tuple(vmem(5)),
        scratch_shapes=[pltpu.SemaphoreType.DMA((2 + CHANNELS // SLICE,))],
        compiler_params=pltpu.CompilerParams(vmem_limit_bytes=66563328),
        name="parcel",
    )(hidden.reshape(tiles, 8, CHANNELS), weight, norm_gain[None], norm_shift[None])
    parcel = lax.ppermute(parcel, "c", [(0, 1), (1, 0)])

    act_shape = (QUAD, WIDE, CELLS, CHANNELS)
    kin_shape = (CLASSES * rows, TAPS, share, SLICE)

    def blank(*shapes):
        return pl.pallas_call(
            lambda *refs: None,
            out_shape=tuple(jax.ShapeDtypeStruct(shape, BF16) for shape in shapes),
            out_specs=tuple(pl.BlockSpec(memory_space=pl.ANY) for _ in shapes),
            compiler_params=room(1),
            name="blank",
        )()

    def ring(step):
        return [(i, (i + step) % chips) for i in range(chips)]

    def activations(parcel, mine, row, gain, shift):
        packed = pl.pallas_call(
            pack_kernel,
            out_shape=jax.ShapeDtypeStruct((chips, 2, width), BF16),
            in_specs=vmem(2),
            out_specs=vmem(1)[0],
            compiler_params=room(6),
            name="pack",
        )(row, parcel)
        tiles = lax.all_to_all(packed, CHIPS, split_axis=0, concat_axis=0, tiled=True)
        active = pl.pallas_call(
            norm_kernel,
            out_shape=jax.ShapeDtypeStruct((WIDE, CELLS, CHANNELS), BF16),
            in_specs=vmem(3),
            out_specs=vmem(1)[0],
            compiler_params=room(6),
            name="norm",
        )(tiles, gain, shift)
        hops = [[(i, i ^ n) for i in range(QUAD)] for n in range(1, QUAD)]
        videos = [active] + [lax.ppermute(active, "gq", hop) for hop in hops]
        return (jnp.stack(videos),) + blank(kin_shape)

    def kernels(parcel, mine, row, gain, shift):
        mine = jnp.concatenate([parcel[:TAPS], mine], axis=1)
        kin = lax.all_gather(mine, "zh", axis=0)
        front, back = kin[: rows // 2], kin[rows // 2 :]
        below = [lax.ppermute(front, CHIPS, ring(1))]
        above = [lax.ppermute(back, CHIPS, ring(-1))]
        below += [lax.ppermute(back, CHIPS, ring(1))]
        above = [lax.ppermute(front, CHIPS, ring(-1))] + above
        low = lax.ppermute(below[0], CHIPS, ring(1))
        high = lax.ppermute(above[1], CHIPS, ring(-1))
        below, above = lax.optimization_barrier([jnp.concatenate(x) for x in (below, above)])
        near = jnp.concatenate([kin, below, above])
        far = jnp.concatenate([low, high])
        near, far = lax.optimization_barrier((near, far))
        return blank(act_shape) + (jnp.concatenate([near, far]),)

    core = lax.axis_index("c")
    active, weights = lax.cond(core == 0, activations, kernels, parcel, mine, row, gain, shift)
    right = [(2 * i, 2 * i + 2) for i in range(chips - 1)]
    left = [(2 * i + 2, 2 * i + 1) for i in range(chips - 1)]
    after = lax.ppermute(active[:, 0], SPACE, left)
    before = lax.ppermute(active[:, WIDE - 1], SPACE, right)
    brought = lax.ppermute(weights, "c", [(1, 0)])
    given = lax.ppermute(active[:, 1:], "c", [(0, 1)])
    columns = jnp.concatenate([before[:, None], active[:, : WIDE - 1]], axis=1)
    given = jnp.concatenate([given, after[:, None]], axis=1)
    bias = conv_bias.astype(F32).reshape(QUAD, SLICE)

    columns = jnp.where(core == 0, columns, given)
    weights = jnp.where(core == 0, brought, weights)
    outs = [None] * QUAD
    for n in reversed(range(QUAD)):
        outs[n] = convolve((n,), columns, weights, bias)[0]
        if n:
            outs[n] = lax.ppermute(outs[n], "gq", [(i, i ^ n) for i in range(QUAD)])
    out = pl.pallas_call(
        spread_kernel,
        out_shape=jax.ShapeDtypeStruct((2 * CELLS, 2 * COLS, CHANNELS), BF16),
        in_specs=vmem(QUAD),
        out_specs=pl.BlockSpec(memory_space=pltpu.HBM),
        scratch_shapes=[pltpu.SemaphoreType.DMA((QUAD,))],
        compiler_params=room(4),
        name="spread",
    )(*outs)
    return out.reshape(FRAMES, 2 * ROWS, 2 * COLS, CHANNELS)


def solution(mesh):
    groups, space = mesh.shape["groups"], mesh.shape["space"]
    torus = Mesh(
        mesh.devices.reshape(groups // QUAD, QUAD, space // (2 * CLASSES), CLASSES, 2),
        ("gh", "gq", "zh", "zl", "c"),
    )
    return jax.shard_map(
        shards,
        mesh=torus,
        in_specs=(
            P(("gh", "gq") + SPACE, None),
            P(),
            P(),
            P(None, None, None, SPACE, None),
            P(),
        ),
        out_specs=P(("gh", "gq"), None, SPACE, None),
        check_vma=False,
    )
```
